32 devices in a mesh: dp: 2 (over x), vblk: 4 (over z), vocab: 4 (over y, core).
Axes of the slice: x: 2, y: 2, z: 4, core: 2. Of those that a mesh axis runs over, the one named last changes fastest.
Arguments:
- hidden: bfloat16 [512, 2048], P('dp'), parts along dimension 0
- w_head: bfloat16 [2048, 256000], P(None, ('vblk', 'vocab'))
- inv_temp: float32 [512], P('dp'), parts along dimension 0
- target: int32 [512], P('dp'), parts along dimension 0
Outputs:
- output 1: float32 [512, 256000], P('dp', ('vblk', 'vocab')), parts along dimension 0
- output 2: float32 [512], P('dp'), parts along dimension 0
There are 2 independent parts. The reference program is written for one: setup_inputs(seed, part) draws one part's arguments, and reference() takes and returns one part's arrays. A program takes and returns all parts, laid end to end along the dimension named above; an argument that names none is the same for every part.
All inputs are finite; a program needn't handle non-finite values.
Results may differ from the reference program's by a relative error of at most 0.001.
Values are sent between devices in bfloat16 or wider.
A program may use at most 1 GiB of HBM per device.

```python
import math
import jax
import jax.numpy as jnp
from jax import lax

D = 2048
V = 256000
ROWS = 256


def setup_inputs(seed: int = 0, part: int = 0) -> dict:
    root_key = jax.random.key(seed)
    key_dir, key_w = jax.random.split(root_key, 2)
    key_h, key_shift, key_temp, key_tgt = jax.random.split(jax.random.fold_in(root_key, part), 4)
    direction = jax.random.normal(key_dir, (D,), jnp.float32)
    direction = direction / jnp.sqrt(jnp.sum(direction * direction))

    def weight_block(block_idx):
        col_ids = (block_idx * 128 + jnp.arange(128)).astype(jnp.float32)
        col_gain = 40.0 + jnp.exp(-8.0 * col_ids / V)
        noise_blk = jax.random.normal(jax.random.fold_in(key_w, block_idx), (D, 128), jnp.float32)
        return (noise_blk * (1.5 / math.sqrt(D)) + direction[:, None] * col_gain[None, :]).astype(jnp.bfloat16)

    w_blocks = lax.map(weight_block, jnp.arange(V // 128))
    w_head = jnp.transpose(w_blocks, (1, 0, 2)).reshape(D, V)
    row_shift = jax.random.uniform(key_shift, (ROWS, 1), jnp.float32, 1.5, 3.5)
    hidden = (jax.random.normal(key_h, (ROWS, D), jnp.float32) + row_shift * direction[None, :]).astype(jnp.bfloat16)
    inv_temp = jax.random.uniform(key_temp, (ROWS,), jnp.float32, 0.75, 1.5)
    target = jax.random.randint(key_tgt, (ROWS,), 0, V, jnp.int32)
    target = target.at[0].set(0).at[ROWS - 1].set(V - 1)
    return {"hidden": hidden, "w_head": w_head, "inv_temp": inv_temp, "target": target}


def reference(hidden, w_head, inv_temp, target):
    logits = jnp.dot(hidden, w_head, preferred_element_type=jnp.float32) * inv_temp[:, None]
    row_max = jnp.max(logits, axis=1, keepdims=True)
    exp_val = jnp.exp(logits - row_max)
    prob_row = exp_val / jnp.sum(exp_val, axis=1, keepdims=True)
    cdf_table = jnp.cumsum(prob_row, axis=1)
    picked = jnp.take_along_axis(cdf_table, target[:, None], axis=1)[:, 0]
    return (cdf_table, picked)
```

```python
import functools

import jax
import jax.numpy as jnp
from jax import lax
from jax.experimental import pallas as pl
from jax.experimental.pallas import tpu as pltpu
from jax.sharding import PartitionSpec as P

F32 = jnp.float32
BF16 = jnp.bfloat16
TW = 1024
BW = 256
NBUF = 4
RG = 32
LOG2E = 1.4426950408889634
NEG = -1e30


def lanes_of(row):
    return jnp.transpose(jnp.broadcast_to(row, (128, 128)))


def row_of(col):
    return jnp.transpose(col)[0:1, :]


def split3(x):
    hi = x.astype(BF16)
    r = x - hi.astype(F32)
    mid = r.astype(BF16)
    lo = (r - mid.astype(F32)).astype(BF16)
    return hi, mid, lo


def block_prefix(x, tri):
    w = x.shape[1]
    t = tri[:w, :w]
    hi, mid, lo = split3(x)
    dot = functools.partial(jnp.dot, preferred_element_type=F32)
    return dot(lo, t) + dot(mid, t) + dot(hi, t)


def fill_triangle(tri):
    i = lax.broadcasted_iota(jnp.int32, (BW, BW), 0)
    j = lax.broadcasted_iota(jnp.int32, (BW, BW), 1)
    tri[...] = jnp.where(i <= j, 1.0, 0.0).astype(BF16)


def blocks_of(width):
    return [(c, min(BW, width - c)) for c in range(0, width, BW)]


def head(cfg, h_hbm, w_hbm, tau_ref, tgt_ref, e_ref, mt_ref, fin_ref, pick_ref,
         h_ref, wbuf, z0, z1, tau, rel, m, s, pk, tri, pay, got, hsem, wsem, send_sem, recv_sem):
    rows, width, nblk, nvoc = cfg
    n = pl.cdiv(width, TW)
    last = width - (n - 1) * TW
    zs = (z0, z1)
    mi, mj = lax.axis_index("vblk"), lax.axis_index("vocab")
    me = mi * nvoc + mj
    group = nblk * nvoc

    def peer(d):
        p = lax.rem(me + d, group)
        return {"vblk": p // nvoc, "vocab": lax.rem(p, nvoc)}

    def w_copy(t, slot, w):
        return pltpu.make_async_copy(
            w_hbm.at[:, pl.ds(pl.multiple_of(t * TW, 128), w)], wbuf.at[slot, :, pl.ds(0, w)], wsem.at[slot])

    h_copy = pltpu.make_async_copy(h_hbm, h_ref, hsem)
    h_copy.start()
    for t in range(min(NBUF - 1, n)):
        w_copy(t, t, TW if t < n - 1 else last).start()

    barrier = pltpu.get_barrier_semaphore()
    for d in range(1, group):
        pl.semaphore_signal(barrier, inc=1, device_id=peer(d), device_id_type=pl.DeviceIdType.MESH)

    base = me * width
    for half in range(rows // 128):
        r = pl.ds(half * 128, 128)
        tau[r, :] = lanes_of(tau_ref[half:half + 1, :] * LOG2E)
        rel[r, :] = lanes_of(tgt_ref[half:half + 1, :] - base)
    m[...] = jnp.full_like(m, NEG)
    s[...] = jnp.zeros_like(s)
    pk[...] = jnp.zeros_like(pk)
    fill_triangle(tri)
    lane = lax.broadcasted_iota(jnp.int32, (RG, 128), 1)

    def process(z, t, w):
        for r0 in range(0, rows, RG):
            r = pl.ds(r0, RG)
            top = z[r, 0:128]
            for c in range(128, w, 128):
                top = jnp.maximum(top, z[r, c:c + 128])
            new = jnp.max(top, axis=1, keepdims=True) * tau[r, :]
            mt_ref[t, r, :] = jnp.maximum(m[r, :], new)
        for r0 in range(0, rows, RG):
            r = pl.ds(r0, RG)
            new, scale = mt_ref[t, r, :], tau[r, :]
            lim = rel[r, :] - t * TW
            total, mass = None, None
            for c in range(0, w, 128):
                e = jnp.exp2(z[r, c:c + 128] * scale - new)
                e_ref[t, r, c:c + 128] = e
                part = jnp.where(lane + c <= lim, e, 0.0)
                total = e if total is None else total + e
                mass = part if mass is None else mass + part
            alpha = jnp.exp2(m[r, :] - new)
            s[r, :] = s[r, :] * alpha + total
            pk[r, :] = pk[r, :] * alpha + mass
            m[r, :] = new

    def logits(z, slot, w):
        z[:, 0:w] = jnp.dot(h_ref[...], wbuf[slot, :, 0:w], preferred_element_type=F32)

    def step(t, parity):
        slot = lax.rem(t, NBUF)
        w_copy(t, slot, TW).wait()

        @pl.when(t + NBUF - 1 < n - 1)
        def _():
            w_copy(t + NBUF - 1, lax.rem(t + NBUF - 1, NBUF), TW).start()

        @pl.when(t + NBUF - 1 == n - 1)
        def _():
            w_copy(n - 1, (n - 1) % NBUF, last).start()

        process(zs[1 - parity], t - 1, TW)
        logits(zs[parity], slot, TW)

    h_copy.wait()
    w_copy(0, 0, TW).wait()
    w_copy(NBUF - 1, NBUF - 1, TW if NBUF < n else last).start()
    logits(z0, 0, TW)

    @pl.loop(0, (n - 2) // 2)
    def _(i):
        step(2 * i + 1, 1)
        step(2 * i + 2, 0)

    w_copy(n - 1, (n - 1) % NBUF, last).wait()
    process(z0, n - 2, TW)
    logits(z1, (n - 1) % NBUF, last)
    process(z1, n - 1, last)

    for half in range(rows // 128):
        r = pl.ds(half * 128, 128)
        ones = jnp.zeros((128, 128), F32)
        pay[half:half + 1, :] = row_of(m[r, :])
        pay[2 + half:3 + half, :] = row_of(jnp.sum(s[r, :], axis=1, keepdims=True) + ones)
        pay[4 + half:5 + half, :] = row_of(jnp.sum(pk[r, :], axis=1, keepdims=True) + ones)
    pl.semaphore_wait(barrier, group - 1)

    def send(d):
        return pltpu.make_async_remote_copy(
            src_ref=pay.at[0:6], dst_ref=got.at[me, 0:6], send_sem=send_sem.at[d], recv_sem=recv_sem.at[me],
            device_id=peer(d), device_id_type=pl.DeviceIdType.MESH)

    def recv(d):
        k = lax.rem(me + d, group)
        return pltpu.make_async_remote_copy(
            src_ref=pay.at[0:6], dst_ref=got.at[k, 0:6], send_sem=send_sem.at[d], recv_sem=recv_sem.at[k],
            device_id=peer(d), device_id_type=pl.DeviceIdType.MESH)

    for d in range(1, group):
        send(d).start()
    got[me, 0:6, :] = pay[0:6, :]

    def prefix(t, w):
        for c, b in blocks_of(w):
            e_ref[t, :, c:c + b] = block_prefix(e_ref[t, :, c:c + b], tri)

    @pl.loop(0, n - 1)
    def _(t):
        prefix(t, TW)

    prefix(n - 1, last)

    for d in range(1, group):
        send(d).wait_send()
        recv(d).wait_recv()

    top = got[0, 0:2, :]
    for k in range(1, group):
        top = jnp.maximum(top, got[k, 0:2, :])
    total = jnp.zeros_like(top)
    lower = jnp.zeros_like(top)
    mass = jnp.zeros_like(top)
    for k in range(group):
        f = jnp.exp2(got[k, 0:2, :] - top)
        part = got[k, 2:4, :] * f
        total += part
        lower += part * jnp.where(k < me, 1.0, 0.0)
        mass += got[k, 4:6, :] * f
    inv = 1.0 / total
    pick_ref[...] = mass * inv
    low = lower * inv
    for half in range(rows // 128):
        r = pl.ds(half * 128, 128)
        fin_ref[0, r, :] = lanes_of(top[half:half + 1, :])
        fin_ref[1, r, :] = lanes_of(inv[half:half + 1, :])
        fin_ref[2, r, :] = lanes_of(low[half:half + 1, :])


def table(cfg, c_ref, mt_ref, fin_ref, mass_ref, out_hbm, pick_ref, stage, off, osem):
    rows, width = cfg
    n = pl.cdiv(width, TW)
    last = width - (n - 1) * TW
    slots = stage.shape[0]
    off[...] = fin_ref[2]
    pick_ref[...] = mass_ref[...]

    def out_copy(t, slot, w):
        return pltpu.make_async_copy(
            stage.at[slot, :, pl.ds(0, w)], out_hbm.at[:, pl.ds(pl.multiple_of(t * TW, 128), w)], osem.at[slot])

    def tile(t, slot, w):
        for r0 in range(0, rows, RG):
            r = pl.ds(r0, RG)
            scale = jnp.exp2(mt_ref[t, r, :] - fin_ref[0, r, :]) * fin_ref[1, r, :]
            o = off[r, :]
            for c, b in blocks_of(w):
                for g in range(c, c + b, 128):
                    v = c_ref[t, r, g:g + 128]
                    stage[slot, r, g:g + 128] = v * scale + o
                o = o + v[:, 127:128] * scale
            off[r, :] = o
        out_copy(t, slot, w).start()

    @pl.loop(0, n - 1)
    def _(t):
        slot = lax.rem(t, slots)

        @pl.when(t >= slots)
        def _():
            out_copy(t - slots, slot, TW).wait()

        tile(t, slot, TW)

    if n - 1 >= slots:
        out_copy(n - 1 - slots, (n - 1) % slots, TW).wait()
    tile(n - 1, (n - 1) % slots, last)
    for t in range(max(0, n - slots), n):
        out_copy(t, t % slots, TW if t < n - 1 else last).wait()


def solution(mesh):
    vocab_axes = ("vblk", "vocab")
    nblk, nvoc = mesh.shape["vblk"], mesh.shape["vocab"]
    group = nblk * nvoc
    any_spec = pl.BlockSpec(memory_space=pl.ANY)
    vmem = pl.BlockSpec(memory_space=pltpu.VMEM)

    def local_step(hidden, w_head, inv_temp, target):
        rows, depth = hidden.shape
        width = w_head.shape[1]
        n = -(-width // TW)
        halves = rows // 128
        e, mt, fin, mass = pl.pallas_call(
            functools.partial(head, (rows, width, nblk, nvoc)),
            name="head",
            out_shape=[
                pltpu.VMEM((n, rows, TW), F32),
                pltpu.VMEM((n, rows, 128), F32),
                pltpu.VMEM((3, rows, 128), F32),
                pltpu.VMEM((halves, 128), F32),
            ],
            in_specs=[any_spec, any_spec, vmem, vmem],
            out_specs=[vmem, vmem, vmem, vmem],
            scratch_shapes=[
                pltpu.VMEM((rows, depth), BF16),
                pltpu.VMEM((NBUF, depth, TW), BF16),
                pltpu.VMEM((rows, TW), F32),
                pltpu.VMEM((rows, TW), F32),
                pltpu.VMEM((rows, 128), F32),
                pltpu.VMEM((rows, 128), jnp.int32),
                pltpu.VMEM((rows, 128), F32),
                pltpu.VMEM((rows, 128), F32),
                pltpu.VMEM((rows, 128), F32),
                pltpu.VMEM((BW, BW), BF16),
                pltpu.VMEM((8, 128), F32),
                pltpu.VMEM((group, 8, 128), F32),
                pltpu.SemaphoreType.DMA,
                pltpu.SemaphoreType.DMA((NBUF,)),
                pltpu.SemaphoreType.DMA((group,)),
                pltpu.SemaphoreType.DMA((group,)),
            ],
            compiler_params=pltpu.CompilerParams(
                collective_id=0, has_side_effects=True, vmem_limit_bytes=36 * 1024 * 1024),
            cost_estimate=pl.CostEstimate(
                flops=2 * rows * depth * width, bytes_accessed=2 * depth * width, transcendentals=rows * width),
        )(hidden, w_head, inv_temp.reshape(halves, 128), target.reshape(halves, 128))
        cdf, pick = pl.pallas_call(
            functools.partial(table, (rows, width)),
            name="table",
            out_shape=[jax.ShapeDtypeStruct((rows, width), F32), jax.ShapeDtypeStruct((halves, 128), F32)],
            in_specs=[vmem] * 4,
            out_specs=[any_spec, vmem],
            scratch_shapes=[
                pltpu.VMEM((4, rows, TW), F32),
                pltpu.VMEM((rows, 128), F32),
                pltpu.SemaphoreType.DMA((4,)),
            ],
            compiler_params=pltpu.CompilerParams(vmem_limit_bytes=12 * 1024 * 1024),
            cost_estimate=pl.CostEstimate(
                flops=4 * rows * width, bytes_accessed=4 * rows * width, transcendentals=0),
        )(e, mt, fin, mass)
        return cdf, pick.reshape(rows)

    return jax.shard_map(local_step, mesh=mesh,
                         in_specs=(P("dp", None), P(None, vocab_axes), P("dp"), P("dp")),
                         out_specs=(P("dp", vocab_axes), P("dp")), check_vma=False)
```

```python
import functools

import jax
import jax.numpy as jnp
from jax import lax
from jax.experimental import pallas as pl
from jax.experimental.pallas import tpu as pltpu
from jax.sharding import PartitionSpec as P

F32 = jnp.float32
BF16 = jnp.bfloat16
TW = 1024
FIRST = 384
LAST = 256
BW = 256
HEAD_MID = 9
SLOTS = 8
NBUF = 4
RG = 32
LOG2E = 1.4426950408889634
NEG = -1e30


def lanes_of(row):
    return jnp.transpose(jnp.broadcast_to(row, (128, 128)))


def row_of(col):
    return jnp.transpose(col)[0:1, :]


def split3(x):
    hi = x.astype(BF16)
    r = x - hi.astype(F32)
    mid = r.astype(BF16)
    lo = (r - mid.astype(F32)).astype(BF16)
    return hi, mid, lo


def block_prefix(x, tri):
    w = x.shape[1]
    t = tri[:w, :w]
    hi, mid, lo = split3(x)
    dot = functools.partial(jnp.dot, preferred_element_type=F32)
    return dot(lo, t) + dot(mid, t) + dot(hi, t)


def fill_triangle(tri):
    i = lax.broadcasted_iota(jnp.int32, (BW, BW), 0)
    j = lax.broadcasted_iota(jnp.int32, (BW, BW), 1)
    tri[...] = jnp.where(i <= j, 1.0, 0.0).astype(BF16)


def tiling(width):
    mid = (width - FIRST - LAST) // TW
    assert FIRST + LAST + mid * TW == width and mid % 2 == 1
    return mid + 2, [FIRST] + [TW] * mid + [LAST], 1 + mid * HEAD_MID // 15


def start_of(t):
    return FIRST + (t - 1) * TW


def blocks_of(width):
    return [(c, min(BW, width - c)) for c in range(0, width, BW)]


def head(cfg, h_hbm, w_hbm, tau_ref, tgt_ref, e_ref, mt_ref, fin_ref, pick_ref,
         h_ref, wbuf, z0, z1, tau, rel, m, s, pk, tri, pay, got, hsem, wsem, send_sem, recv_sem):
    rows, width, nblk, nvoc = cfg
    n, widths, formed = tiling(width)
    zs = (z0, z1)
    mi, mj = lax.axis_index("vblk"), lax.axis_index("vocab")
    me = mi * nvoc + mj
    group = nblk * nvoc

    def peer(d):
        p = lax.rem(me + d, group)
        return {"vblk": p // nvoc, "vocab": lax.rem(p, nvoc)}

    def w_copy(t, slot, w):
        return pltpu.make_async_copy(
            w_hbm.at[:, pl.ds(0 if w == FIRST else pl.multiple_of(start_of(t), 128), w)], wbuf.at[slot, :, pl.ds(0, w)], wsem.at[slot])

    h_copy = pltpu.make_async_copy(h_hbm, h_ref, hsem)
    h_copy.start()
    for t in range(min(NBUF - 1, n)):
        w_copy(t, t, widths[t]).start()

    barrier = pltpu.get_barrier_semaphore()
    for d in range(1, group):
        pl.semaphore_signal(barrier, inc=1, device_id=peer(d), device_id_type=pl.DeviceIdType.MESH)

    base = me * width
    for half in range(rows // 128):
        r = pl.ds(half * 128, 128)
        tau[r, :] = lanes_of(tau_ref[half:half + 1, :] * LOG2E)
        rel[r, :] = lanes_of(tgt_ref[half:half + 1, :] - base)
    m[...] = jnp.full_like(m, NEG)
    s[...] = jnp.zeros_like(s)
    pk[...] = jnp.zeros_like(pk)
    fill_triangle(tri)
    lane = lax.broadcasted_iota(jnp.int32, (RG, 128), 1)

    def process(z, t, w):
        for r0 in range(0, rows, RG):
            r = pl.ds(r0, RG)
            top = z[r, 0:128]
            for c in range(128, w, 128):
                top = jnp.maximum(top, z[r, c:c + 128])
            new = jnp.max(top, axis=1, keepdims=True) * tau[r, :]
            mt_ref[t, r, :] = jnp.maximum(m[r, :], new)
        for r0 in range(0, rows, RG):
            r = pl.ds(r0, RG)
            new, scale = mt_ref[t, r, :], tau[r, :]
            lim = rel[r, :] - (0 if w == FIRST else start_of(t))
            total, mass = None, None
            for c in range(0, w, 128):
                e = jnp.exp2(z[r, c:c + 128] * scale - new)
                e_ref[t, r, c:c + 128] = e
                part = jnp.where(lane + c <= lim, e, 0.0)
                total = e if total is None else total + e
                mass = part if mass is None else mass + part
            alpha = jnp.exp2(m[r, :] - new)
            s[r, :] = s[r, :] * alpha + total
            pk[r, :] = pk[r, :] * alpha + mass
            m[r, :] = new

    def logits(z, slot, w):
        dot = functools.partial(jnp.dot, preferred_element_type=F32)
        if w > BW:
            z[:, 0:w] = dot(h_ref[...], wbuf[slot, :, 0:w])
        else:
            k = h_ref.shape[1] // 2
            z[:, 0:w] = dot(h_ref[:, :k], wbuf[slot, :k, 0:w]) + dot(h_ref[:, k:], wbuf[slot, k:, 0:w])

    def step(t, parity):
        slot = lax.rem(t, NBUF)
        w_copy(t, slot, TW).wait()
        ahead = t + NBUF - 1

        @pl.when(ahead < n - 1)
        def _():
            w_copy(ahead, lax.rem(ahead, NBUF), TW).start()

        @pl.when(ahead == n - 1)
        def _():
            w_copy(n - 1, (n - 1) % NBUF, LAST).start()

        process(zs[1 - parity], t - 1, TW)
        logits(zs[parity], slot, TW)

    h_copy.wait()
    w_copy(0, 0, FIRST).wait()
    w_copy(NBUF - 1, NBUF - 1, widths[NBUF - 1]).start()
    logits(z0, 0, FIRST)
    w_copy(1, 1, TW).wait()
    if NBUF < n:
        w_copy(NBUF, 0, widths[NBUF]).start()
    process(z0, 0, FIRST)
    logits(z1, 1, TW)

    @pl.loop(0, (n - 3) // 2)
    def _(i):
        step(2 * i + 2, 0)
        step(2 * i + 3, 1)

    w_copy(n - 1, (n - 1) % NBUF, LAST).wait()
    process(zs[n % 2], n - 2, TW)
    logits(zs[(n - 1) % 2], (n - 1) % NBUF, LAST)
    process(zs[(n - 1) % 2], n - 1, LAST)

    for half in range(rows // 128):
        r = pl.ds(half * 128, 128)
        ones = jnp.zeros((128, 128), F32)
        pay[half:half + 1, :] = row_of(m[r, :])
        pay[2 + half:3 + half, :] = row_of(jnp.sum(s[r, :], axis=1, keepdims=True) + ones)
        pay[4 + half:5 + half, :] = row_of(jnp.sum(pk[r, :], axis=1, keepdims=True) + ones)
    pl.semaphore_wait(barrier, group - 1)

    def send(d):
        return pltpu.make_async_remote_copy(
            src_ref=pay.at[0:6], dst_ref=got.at[me, 0:6], send_sem=send_sem.at[d], recv_sem=recv_sem.at[me],
            device_id=peer(d), device_id_type=pl.DeviceIdType.MESH)

    def recv(d):
        k = lax.rem(me + d, group)
        return pltpu.make_async_remote_copy(
            src_ref=pay.at[0:6], dst_ref=got.at[k, 0:6], send_sem=send_sem.at[d], recv_sem=recv_sem.at[k],
            device_id=peer(d), device_id_type=pl.DeviceIdType.MESH)

    for d in range(1, group):
        send(d).start()
    got[me, 0:6, :] = pay[0:6, :]

    def prefix(t, w):
        for c, b in blocks_of(w):
            e_ref[t, :, c:c + b] = block_prefix(e_ref[t, :, c:c + b], tri)

    prefix(0, FIRST)

    @pl.loop(1, formed)
    def _(t):
        prefix(t, TW)

    for d in range(1, group):
        send(d).wait_send()
        recv(d).wait_recv()

    top = got[0, 0:2, :]
    for k in range(1, group):
        top = jnp.maximum(top, got[k, 0:2, :])
    total = jnp.zeros_like(top)
    lower = jnp.zeros_like(top)
    mass = jnp.zeros_like(top)
    for k in range(group):
        f = jnp.exp2(got[k, 0:2, :] - top)
        part = got[k, 2:4, :] * f
        total += part
        lower += part * jnp.where(k < me, 1.0, 0.0)
        mass += got[k, 4:6, :] * f
    inv = 1.0 / total
    pick_ref[...] = mass * inv
    low = lower * inv
    for half in range(rows // 128):
        r = pl.ds(half * 128, 128)
        fin_ref[0, r, :] = lanes_of(top[half:half + 1, :])
        fin_ref[1, r, :] = lanes_of(inv[half:half + 1, :])
        fin_ref[2, r, :] = lanes_of(low[half:half + 1, :])


def table(cfg, c_ref, mt_ref, fin_ref, mass_ref, out_hbm, pick_ref, stage, head_stage, tail_stage, off, tri, osem):
    rows, width = cfg
    n, widths, formed = tiling(width)
    slots = stage.shape[0]
    off[...] = fin_ref[2]
    pick_ref[...] = mass_ref[...]
    fill_triangle(tri)

    def slot_of(t):
        return lax.rem(t - 1, slots)

    def out_copy(t, w):
        buf = head_stage if w == FIRST else tail_stage if w == LAST else stage.at[slot_of(t)]
        sem = osem.at[slots] if w == FIRST else osem.at[slots + 1] if w == LAST else osem.at[slot_of(t)]
        col = 0 if w == FIRST else pl.multiple_of(start_of(t), 128)
        return pltpu.make_async_copy(buf, out_hbm.at[:, pl.ds(col, w)], sem)

    def finish(t, w, ready):
        buf = head_stage if w == FIRST else tail_stage if w == LAST else stage.at[slot_of(t)]
        for c, b in blocks_of(w):
            if not ready:
                buf[:, c:c + b] = block_prefix(c_ref[t, :, c:c + b], tri)
            for r0 in range(0, rows, RG):
                r = pl.ds(r0, RG)
                scale = jnp.exp2(mt_ref[t, r, :] - fin_ref[0, r, :]) * fin_ref[1, r, :]
                o = off[r, :]
                for g in range(c, c + b, 128):
                    v = c_ref[t, r, g:g + 128] if ready else buf[r, g:g + 128]
                    buf[r, g:g + 128] = v * scale + o
                off[r, :] = o + v[:, 127:128] * scale
        out_copy(t, w).start()

    def middle(lo, hi, ready):
        @pl.loop(lo, hi)
        def _(t):
            @pl.when(t > slots)
            def _():
                out_copy(t - slots, TW).wait()

            finish(t, TW, ready)

    finish(0, FIRST, True)
    middle(1, formed, True)
    middle(formed, n - 1, False)
    finish(n - 1, LAST, False)
    out_copy(0, FIRST).wait()
    for t in range(max(1, n - 1 - slots), n - 1):
        out_copy(t, TW).wait()
    out_copy(n - 1, LAST).wait()


def solution(mesh):
    vocab_axes = ("vblk", "vocab")
    nblk, nvoc = mesh.shape["vblk"], mesh.shape["vocab"]
    group = nblk * nvoc
    any_spec = pl.BlockSpec(memory_space=pl.ANY)
    vmem = pl.BlockSpec(memory_space=pltpu.VMEM)

    def local_step(hidden, w_head, inv_temp, target):
        rows, depth = hidden.shape
        width = w_head.shape[1]
        n = tiling(width)[0]
        halves = rows // 128
        e, mt, fin, mass = pl.pallas_call(
            functools.partial(head, (rows, width, nblk, nvoc)),
            name="head",
            out_shape=[
                pltpu.VMEM((n, rows, TW), F32),
                pltpu.VMEM((n, rows, 128), F32),
                pltpu.VMEM((3, rows, 128), F32),
                pltpu.VMEM((halves, 128), F32),
            ],
            in_specs=[any_spec, any_spec, vmem, vmem],
            out_specs=[vmem, vmem, vmem, vmem],
            scratch_shapes=[
                pltpu.VMEM((rows, depth), BF16),
                pltpu.VMEM((NBUF, depth, TW), BF16),
                pltpu.VMEM((rows, TW), F32),
                pltpu.VMEM((rows, TW), F32),
                pltpu.VMEM((rows, 128), F32),
                pltpu.VMEM((rows, 128), jnp.int32),
                pltpu.VMEM((rows, 128), F32),
                pltpu.VMEM((rows, 128), F32),
                pltpu.VMEM((rows, 128), F32),
                pltpu.VMEM((BW, BW), BF16),
                pltpu.VMEM((8, 128), F32),
                pltpu.VMEM((group, 8, 128), F32),
                pltpu.SemaphoreType.DMA,
                pltpu.SemaphoreType.DMA((NBUF,)),
                pltpu.SemaphoreType.DMA((group,)),
                pltpu.SemaphoreType.DMA((group,)),
            ],
            compiler_params=pltpu.CompilerParams(
                collective_id=0, has_side_effects=True,
                vmem_limit_bytes=36 * 1024 * 1024),
            cost_estimate=pl.CostEstimate(
                flops=2 * rows * depth * width, bytes_accessed=2 * depth * width, transcendentals=rows * width),
        )(hidden, w_head, inv_temp.reshape(halves, 128), target.reshape(halves, 128))
        cdf, pick = pl.pallas_call(
            functools.partial(table, (rows, width)),
            name="table",
            out_shape=[jax.ShapeDtypeStruct((rows, width), F32), jax.ShapeDtypeStruct((halves, 128), F32)],
            in_specs=[vmem] * 4,
            out_specs=[any_spec, vmem],
            scratch_shapes=[
                pltpu.VMEM((SLOTS, rows, TW), F32),
                pltpu.VMEM((rows, FIRST), F32),
                pltpu.VMEM((rows, LAST), F32),
                pltpu.VMEM((rows, 128), F32),
                pltpu.VMEM((BW, BW), BF16),
                pltpu.SemaphoreType.DMA((SLOTS + 2,)),
            ],
            compiler_params=pltpu.CompilerParams(vmem_limit_bytes=13 * 1024 * 1024),
            cost_estimate=pl.CostEstimate(
                flops=4 * rows * width, bytes_accessed=4 * rows * width, transcendentals=0),
        )(e, mt, fin, mass)
        return cdf, pick.reshape(rows)

    return jax.shard_map(local_step, mesh=mesh,
                         in_specs=(P("dp", None), P(None, vocab_axes), P("dp"), P("dp")),
                         out_specs=(P("dp", vocab_axes), P("dp")), check_vma=False)
```

```python
import functools

import jax
import jax.numpy as jnp
from jax import lax
from jax.experimental import pallas as pl
from jax.experimental.pallas import tpu as pltpu
from jax.sharding import PartitionSpec as P

F32 = jnp.float32
BF16 = jnp.bfloat16
TW = 1024
FIRST = 384
LAST = 256
BW = 256
HEAD_MID = 12
SLOTS = 8
NBUF = 4
RG = 32
LOG2E = 1.4426950408889634
NEG = -1e30


def lanes_of(row):
    return jnp.transpose(jnp.broadcast_to(row, (128, 128)))


def row_of(col):
    return jnp.transpose(col)[0:1, :]


def split3(x):
    hi = x.astype(BF16)
    r = x - hi.astype(F32)
    mid = r.astype(BF16)
    lo = (r - mid.astype(F32)).astype(BF16)
    return hi, mid, lo


def block_prefix(x, tri):
    w = x.shape[1]
    t = tri[:w, :w]
    hi, mid, lo = split3(x)
    dot = functools.partial(jnp.dot, preferred_element_type=F32)
    return dot(lo, t) + dot(mid, t) + dot(hi, t)


def fill_triangle(tri):
    i = lax.broadcasted_iota(jnp.int32, (BW, BW), 0)
    j = lax.broadcasted_iota(jnp.int32, (BW, BW), 1)
    tri[...] = jnp.where(i <= j, 1.0, 0.0).astype(BF16)


def tiling(width):
    mid = (width - FIRST - LAST) // TW
    assert FIRST + LAST + mid * TW == width and mid % 2 == 1
    return mid + 2, [FIRST] + [TW] * mid + [LAST], 1 + mid * HEAD_MID // 15


def start_of(t):
    return FIRST + (t - 1) * TW


def blocks_of(width):
    return [(c, min(BW, width - c)) for c in range(0, width, BW)]


def head(cfg, h_hbm, w_hbm, tau_ref, tgt_ref, e_ref, mt_ref, fin_ref, pick_ref,
         h_ref, wbuf, z0, z1, tau, rel, m, s, pk, tri, pay, got, hsem, wsem, send_sem, recv_sem):
    rows, width, nblk, nvoc = cfg
    n, widths, formed = tiling(width)
    zs = (z0, z1)
    mi, mj = lax.axis_index("vblk"), lax.axis_index("vocab")
    me = mi * nvoc + mj
    group = nblk * nvoc

    def peer(d):
        p = lax.rem(me + d, group)
        return {"vblk": p // nvoc, "vocab": lax.rem(p, nvoc)}

    def w_copy(t, slot, w):
        return pltpu.make_async_copy(
            w_hbm.at[:, pl.ds(0 if w == FIRST else pl.multiple_of(start_of(t), 128), w)], wbuf.at[slot, :, pl.ds(0, w)], wsem.at[slot])

    h_copy = pltpu.make_async_copy(h_hbm, h_ref, hsem)
    h_copy.start()
    for t in range(min(NBUF, n)):
        w_copy(t, t, widths[t]).start()

    barrier = pltpu.get_barrier_semaphore()
    for d in range(1, group):
        pl.semaphore_signal(barrier, inc=1, device_id=peer(d), device_id_type=pl.DeviceIdType.MESH)

    base = me * width
    for half in range(rows // 128):
        r = pl.ds(half * 128, 128)
        tau[r, :] = lanes_of(tau_ref[half:half + 1, :] * LOG2E)
        rel[r, :] = lanes_of(tgt_ref[half:half + 1, :] - base)
    m[...] = jnp.full_like(m, NEG)
    s[...] = jnp.zeros_like(s)
    pk[...] = jnp.zeros_like(pk)
    fill_triangle(tri)
    lane = lax.broadcasted_iota(jnp.int32, (RG, 128), 1)

    def process(z, t, w):
        for r0 in range(0, rows, RG):
            r = pl.ds(r0, RG)
            top = z[r, 0:128]
            for c in range(128, w, 128):
                top = jnp.maximum(top, z[r, c:c + 128])
            new = jnp.max(top, axis=1, keepdims=True) * tau[r, :]
            mt_ref[t, r, :] = jnp.maximum(m[r, :], new)
        for r0 in range(0, rows, RG):
            r = pl.ds(r0, RG)
            new, scale = mt_ref[t, r, :], tau[r, :]
            lim = rel[r, :] - (0 if w == FIRST else start_of(t))
            total, mass = None, None
            for c in range(0, w, 128):
                e = jnp.exp2(z[r, c:c + 128] * scale - new)
                e_ref[t, r, c:c + 128] = e
                part = jnp.where(lane + c <= lim, e, 0.0)
                total = e if total is None else total + e
                mass = part if mass is None else mass + part
            alpha = jnp.exp2(m[r, :] - new)
            s[r, :] = s[r, :] * alpha + total
            pk[r, :] = pk[r, :] * alpha + mass
            m[r, :] = new

    def logits(z, slot, w):
        dot = functools.partial(jnp.dot, preferred_element_type=F32)
        if w > BW:
            z[:, 0:w] = dot(h_ref[...], wbuf[slot, :, 0:w])
        else:
            k = h_ref.shape[1] // 2
            z[:, 0:w] = dot(h_ref[:, :k], wbuf[slot, :k, 0:w]) + dot(h_ref[:, k:], wbuf[slot, k:, 0:w])

    h_copy.wait()
    w_copy(0, 0, FIRST).wait()
    logits(z0, 0, FIRST)
    w_copy(1, 1, TW).wait()
    process(z0, 0, FIRST)
    logits(z1, 1, TW)

    @pl.loop(0, (n - 3) // 2)
    def _(i):
        t = 2 * i + 2
        slot, free = lax.rem(t, NBUF), lax.rem(t + 2, NBUF)

        @pl.when(t + 2 < n - 1)
        def _():
            w_copy(t + 2, free, TW).start()
            w_copy(t + 3, free + 1, TW).start()

        @pl.when(t + 2 == n - 1)
        def _():
            w_copy(n - 1, (n - 1) % NBUF, LAST).start()

        w_copy(t, slot, TW).wait()
        w_copy(t + 1, slot + 1, TW).wait()
        process(z1, t - 1, TW)
        logits(z0, slot, TW)
        process(z0, t, TW)
        logits(z1, slot + 1, TW)

    w_copy(n - 1, (n - 1) % NBUF, LAST).wait()
    process(zs[n % 2], n - 2, TW)
    logits(zs[(n - 1) % 2], (n - 1) % NBUF, LAST)
    process(zs[(n - 1) % 2], n - 1, LAST)

    for half in range(rows // 128):
        r = pl.ds(half * 128, 128)
        ones = jnp.zeros((128, 128), F32)
        pay[half:half + 1, :] = row_of(m[r, :])
        pay[2 + half:3 + half, :] = row_of(jnp.sum(s[r, :], axis=1, keepdims=True) + ones)
        pay[4 + half:5 + half, :] = row_of(jnp.sum(pk[r, :], axis=1, keepdims=True) + ones)
    pl.semaphore_wait(barrier, group - 1)

    def send(d):
        return pltpu.make_async_remote_copy(
            src_ref=pay.at[0:6], dst_ref=got.at[me, 0:6], send_sem=send_sem.at[d], recv_sem=recv_sem.at[me],
            device_id=peer(d), device_id_type=pl.DeviceIdType.MESH)

    def recv(d):
        k = lax.rem(me + d, group)
        return pltpu.make_async_remote_copy(
            src_ref=pay.at[0:6], dst_ref=got.at[k, 0:6], send_sem=send_sem.at[d], recv_sem=recv_sem.at[k],
            device_id=peer(d), device_id_type=pl.DeviceIdType.MESH)

    for d in sorted(range(1, group), key=lambda d: -min(d, group - d)):
        send(d).start()
    got[me, 0:6, :] = pay[0:6, :]

    def prefix(t, w):
        for c, b in blocks_of(w):
            e_ref[t, :, c:c + b] = block_prefix(e_ref[t, :, c:c + b], tri)

    prefix(0, FIRST)
    if formed % 2 == 0:
        prefix(1, TW)

    @pl.loop(0, (formed - 1) // 2)
    def _(i):
        t = 2 * i + 2 - formed % 2
        prefix(t, TW)
        prefix(t + 1, TW)

    for d in range(1, group):
        send(d).wait_send()
        recv(d).wait_recv()

    top = got[0, 0:2, :]
    for k in range(1, group):
        top = jnp.maximum(top, got[k, 0:2, :])
    total = jnp.zeros_like(top)
    lower = jnp.zeros_like(top)
    mass = jnp.zeros_like(top)
    for k in range(group):
        f = jnp.exp2(got[k, 0:2, :] - top)
        part = got[k, 2:4, :] * f
        total += part
        lower += part * jnp.where(k < me, 1.0, 0.0)
        mass += got[k, 4:6, :] * f
    inv = 1.0 / total
    pick_ref[...] = mass * inv
    low = lower * inv
    for half in range(rows // 128):
        r = pl.ds(half * 128, 128)
        fin_ref[0, r, :] = lanes_of(top[half:half + 1, :])
        fin_ref[1, r, :] = lanes_of(inv[half:half + 1, :])
        fin_ref[2, r, :] = lanes_of(low[half:half + 1, :])


def table(cfg, c_ref, mt_ref, fin_ref, mass_ref, out_hbm, pick_ref, stage, head_stage, tail_stage, off, tri, osem):
    rows, width = cfg
    n, widths, formed = tiling(width)
    slots = stage.shape[0]
    off[...] = fin_ref[2]
    pick_ref[...] = mass_ref[...]
    fill_triangle(tri)

    def slot_of(t):
        return lax.rem(t - 1, slots)

    def out_copy(t, w):
        buf = head_stage if w == FIRST else tail_stage if w == LAST else stage.at[slot_of(t)]
        sem = osem.at[slots] if w == FIRST else osem.at[slots + 1] if w == LAST else osem.at[slot_of(t)]
        col = 0 if w == FIRST else pl.multiple_of(start_of(t), 128)
        return pltpu.make_async_copy(buf, out_hbm.at[:, pl.ds(col, w)], sem)

    def finish(t, w, ready):
        buf = head_stage if w == FIRST else tail_stage if w == LAST else stage.at[slot_of(t)]
        for c, b in blocks_of(w):
            if not ready:
                buf[:, c:c + b] = block_prefix(c_ref[t, :, c:c + b], tri)
            for r0 in range(0, rows, RG):
                r = pl.ds(r0, RG)
                scale = jnp.exp2(mt_ref[t, r, :] - fin_ref[0, r, :]) * fin_ref[1, r, :]
                o = off[r, :]
                for g in range(c, c + b, 128):
                    v = c_ref[t, r, g:g + 128] if ready else buf[r, g:g + 128]
                    buf[r, g:g + 128] = v * scale + o
                off[r, :] = o + v[:, 127:128] * scale
        out_copy(t, w).start()

    def middle(lo, hi, ready):
        @pl.loop(lo, hi)
        def _(t):
            @pl.when(t > slots)
            def _():
                out_copy(t - slots, TW).wait()

            finish(t, TW, ready)

    finish(0, FIRST, True)
    middle(1, formed, True)
    middle(formed, n - 1, False)
    finish(n - 1, LAST, False)
    out_copy(0, FIRST).wait()
    for t in range(max(1, n - 1 - slots), n - 1):
        out_copy(t, TW).wait()
    out_copy(n - 1, LAST).wait()


def solution(mesh):
    vocab_axes = ("vblk", "vocab")
    nblk, nvoc = mesh.shape["vblk"], mesh.shape["vocab"]
    group = nblk * nvoc
    any_spec = pl.BlockSpec(memory_space=pl.ANY)
    vmem = pl.BlockSpec(memory_space=pltpu.VMEM)

    def local_step(hidden, w_head, inv_temp, target):
        rows, depth = hidden.shape
        width = w_head.shape[1]
        n = tiling(width)[0]
        halves = rows // 128
        e, mt, fin, mass = pl.pallas_call(
            functools.partial(head, (rows, width, nblk, nvoc)),
            name="head",
            out_shape=[
                pltpu.VMEM((n, rows, TW), F32),
                pltpu.VMEM((n, rows, 128), F32),
                pltpu.VMEM((3, rows, 128), F32),
                pltpu.VMEM((halves, 128), F32),
            ],
            in_specs=[any_spec, any_spec, vmem, vmem],
            out_specs=[vmem, vmem, vmem, vmem],
            scratch_shapes=[
                pltpu.VMEM((rows, depth), BF16),
                pltpu.VMEM((NBUF, depth, TW), BF16),
                pltpu.VMEM((rows, TW), F32),
                pltpu.VMEM((rows, TW), F32),
                pltpu.VMEM((rows, 128), F32),
                pltpu.VMEM((rows, 128), jnp.int32),
                pltpu.VMEM((rows, 128), F32),
                pltpu.VMEM((rows, 128), F32),
                pltpu.VMEM((rows, 128), F32),
                pltpu.VMEM((BW, BW), BF16),
                pltpu.VMEM((8, 128), F32),
                pltpu.VMEM((group, 8, 128), F32),
                pltpu.SemaphoreType.DMA,
                pltpu.SemaphoreType.DMA((NBUF,)),
                pltpu.SemaphoreType.DMA((group,)),
                pltpu.SemaphoreType.DMA((group,)),
            ],
            compiler_params=pltpu.CompilerParams(
                collective_id=0, has_side_effects=True,
                vmem_limit_bytes=36 * 1024 * 1024),
            cost_estimate=pl.CostEstimate(
                flops=2 * rows * depth * width, bytes_accessed=2 * depth * width, transcendentals=rows * width),
        )(hidden, w_head, inv_temp.reshape(halves, 128), target.reshape(halves, 128))
        cdf, pick = pl.pallas_call(
            functools.partial(table, (rows, width)),
            name="table",
            out_shape=[jax.ShapeDtypeStruct((rows, width), F32), jax.ShapeDtypeStruct((halves, 128), F32)],
            in_specs=[vmem] * 4,
            out_specs=[any_spec, vmem],
            scratch_shapes=[
                pltpu.VMEM((SLOTS, rows, TW), F32),
                pltpu.VMEM((rows, FIRST), F32),
                pltpu.VMEM((rows, LAST), F32),
                pltpu.VMEM((rows, 128), F32),
                pltpu.VMEM((BW, BW), BF16),
                pltpu.SemaphoreType.DMA((SLOTS + 2,)),
            ],
            compiler_params=pltpu.CompilerParams(vmem_limit_bytes=13 * 1024 * 1024),
            cost_estimate=pl.CostEstimate(
                flops=4 * rows * width, bytes_accessed=4 * rows * width, transcendentals=0),
        )(e, mt, fin, mass)
        return cdf, pick.reshape(rows)

    return jax.shard_map(local_step, mesh=mesh,
                         in_specs=(P("dp", None), P(None, vocab_axes), P("dp"), P("dp")),
                         out_specs=(P("dp", vocab_axes), P("dp")), check_vma=False)
```

```python
import functools

import jax
import jax.numpy as jnp
from jax import lax
from jax.experimental import pallas as pl
from jax.experimental.pallas import tpu as pltpu
from jax.sharding import PartitionSpec as P

F32 = jnp.float32
BF16 = jnp.bfloat16
TW = 1024
FIRST = 384
LAST = 256
BW = 256
HEAD_MID = 12
SLOTS = 8
NBUF = 4
CUTS = 4
RG = 32
LOG2E = 1.4426950408889634
NEG = -1e30


def lanes_of(row):
    return jnp.transpose(jnp.broadcast_to(row, (128, 128)))


def row_of(col):
    return jnp.transpose(col)[0:1, :]


def split3(x):
    hi = x.astype(BF16)
    r = x - hi.astype(F32)
    mid = r.astype(BF16)
    lo = (r - mid.astype(F32)).astype(BF16)
    return hi, mid, lo


def block_prefix(x, tri):
    w = x.shape[1]
    t = tri[:w, :w]
    hi, mid, lo = split3(x)
    dot = functools.partial(jnp.dot, preferred_element_type=F32)
    return dot(lo, t) + dot(mid, t) + dot(hi, t)


def fill_triangle(tri):
    i = lax.broadcasted_iota(jnp.int32, (BW, BW), 0)
    j = lax.broadcasted_iota(jnp.int32, (BW, BW), 1)
    tri[...] = jnp.where(i <= j, 1.0, 0.0).astype(BF16)


def tiling(width):
    mid = (width - FIRST - LAST) // TW
    assert FIRST + LAST + mid * TW == width and mid % 2 == 1
    return mid + 2, [FIRST] + [TW] * mid + [LAST], 1 + mid * HEAD_MID // 15


def start_of(t):
    return FIRST + (t - 1) * TW


def blocks_of(width):
    return [(c, min(BW, width - c)) for c in range(0, width, BW)]


def head(cfg, h_hbm, w_hbm, tau_ref, tgt_ref, e_ref, mt_ref, fin_ref, pick_ref,
         h_ref, wbuf, z0, z1, tau, rel, m, s, pk, tri, pay, got, hsem, wsem, send_sem, recv_sem):
    rows, width, nblk, nvoc = cfg
    n, widths, formed = tiling(width)
    zs = (z0, z1)
    mi, mj = lax.axis_index("vblk"), lax.axis_index("vocab")
    me = mi * nvoc + mj
    group = nblk * nvoc

    def peer(d):
        p = lax.rem(me + d, group)
        return {"vblk": p // nvoc, "vocab": lax.rem(p, nvoc)}

    def w_copy(t, slot, w, k0=0, k=None):
        col = 0 if w == FIRST else pl.multiple_of(start_of(t), 128)
        k = w_hbm.shape[0] if k is None else k
        return pltpu.make_async_copy(
            w_hbm.at[pl.ds(k0, k), pl.ds(col, w)], wbuf.at[slot, pl.ds(k0, k), pl.ds(0, w)], wsem.at[slot])

    def w_start(t, slot, w):
        k = w_hbm.shape[0] // CUTS
        for i in range(CUTS):
            w_copy(t, slot, w, i * k, k).start()

    def w_wait(t, slot, w):
        w_copy(t, slot, w).wait()

    h_copy = pltpu.make_async_copy(h_hbm, h_ref, hsem)
    h_copy.start()
    for t in range(min(NBUF, n)):
        w_start(t, t, widths[t])

    barrier = pltpu.get_barrier_semaphore()
    for d in range(1, group):
        pl.semaphore_signal(barrier, inc=1, device_id=peer(d), device_id_type=pl.DeviceIdType.MESH)

    base = me * width
    for half in range(rows // 128):
        r = pl.ds(half * 128, 128)
        tau[r, :] = lanes_of(tau_ref[half:half + 1, :] * LOG2E)
        rel[r, :] = lanes_of(tgt_ref[half:half + 1, :] - base)
    m[...] = jnp.full_like(m, NEG)
    s[...] = jnp.zeros_like(s)
    pk[...] = jnp.zeros_like(pk)
    fill_triangle(tri)
    lane = lax.broadcasted_iota(jnp.int32, (RG, 128), 1)

    def process(z, t, w):
        for r0 in range(0, rows, RG):
            r = pl.ds(r0, RG)
            top = z[r, 0:128]
            for c in range(128, w, 128):
                top = jnp.maximum(top, z[r, c:c + 128])
            new = jnp.max(top, axis=1, keepdims=True) * tau[r, :]
            mt_ref[t, r, :] = jnp.maximum(m[r, :], new)
        for r0 in range(0, rows, RG):
            r = pl.ds(r0, RG)
            new, scale = mt_ref[t, r, :], tau[r, :]
            lim = rel[r, :] - (0 if w == FIRST else start_of(t))
            total, mass = None, None
            for c in range(0, w, 128):
                e = jnp.exp2(z[r, c:c + 128] * scale - new)
                e_ref[t, r, c:c + 128] = e
                part = jnp.where(lane + c <= lim, e, 0.0)
                total = e if total is None else total + e
                mass = part if mass is None else mass + part
            alpha = jnp.exp2(m[r, :] - new)
            s[r, :] = s[r, :] * alpha + total
            pk[r, :] = pk[r, :] * alpha + mass
            m[r, :] = new

    def logits(z, slot, w):
        dot = functools.partial(jnp.dot, preferred_element_type=F32)
        if w > BW:
            z[:, 0:w] = dot(h_ref[...], wbuf[slot, :, 0:w])
        else:
            k = h_ref.shape[1] // 2
            z[:, 0:w] = dot(h_ref[:, :k], wbuf[slot, :k, 0:w]) + dot(h_ref[:, k:], wbuf[slot, k:, 0:w])

    def step(t, parity):
        slot = lax.rem(t, NBUF)
        w_wait(t, slot, TW)
        ahead = t + NBUF - 1

        @pl.when(ahead < n - 1)
        def _():
            w_start(ahead, lax.rem(ahead, NBUF), TW)

        @pl.when(ahead == n - 1)
        def _():
            w_start(n - 1, (n - 1) % NBUF, LAST)

        process(zs[1 - parity], t - 1, TW)
        logits(zs[parity], slot, TW)

    h_copy.wait()
    w_wait(0, 0, FIRST)
    logits(z0, 0, FIRST)
    w_wait(1, 1, TW)
    if NBUF < n:
        w_start(NBUF, 0, widths[NBUF])
    process(z0, 0, FIRST)
    logits(z1, 1, TW)

    @pl.loop(0, (n - 3) // 2)
    def _(i):
        step(2 * i + 2, 0)
        step(2 * i + 3, 1)

    w_wait(n - 1, (n - 1) % NBUF, LAST)
    process(zs[n % 2], n - 2, TW)
    logits(zs[(n - 1) % 2], (n - 1) % NBUF, LAST)
    process(zs[(n - 1) % 2], n - 1, LAST)

    for half in range(rows // 128):
        r = pl.ds(half * 128, 128)
        ones = jnp.zeros((128, 128), F32)
        pay[half:half + 1, :] = row_of(m[r, :])
        pay[2 + half:3 + half, :] = row_of(jnp.sum(s[r, :], axis=1, keepdims=True) + ones)
        pay[4 + half:5 + half, :] = row_of(jnp.sum(pk[r, :], axis=1, keepdims=True) + ones)
    pl.semaphore_wait(barrier, group - 1)

    def send(d):
        return pltpu.make_async_remote_copy(
            src_ref=pay.at[0:6], dst_ref=got.at[me, 0:6], send_sem=send_sem.at[d], recv_sem=recv_sem.at[me],
            device_id=peer(d), device_id_type=pl.DeviceIdType.MESH)

    def recv(d):
        k = lax.rem(me + d, group)
        return pltpu.make_async_remote_copy(
            src_ref=pay.at[0:6], dst_ref=got.at[k, 0:6], send_sem=send_sem.at[d], recv_sem=recv_sem.at[k],
            device_id=peer(d), device_id_type=pl.DeviceIdType.MESH)

    for d in sorted(range(1, group), key=lambda d: -min(d, group - d)):
        send(d).start()
    got[me, 0:6, :] = pay[0:6, :]

    def prefix(t, w):
        for c, b in blocks_of(w):
            e_ref[t, :, c:c + b] = block_prefix(e_ref[t, :, c:c + b], tri)

    prefix(0, FIRST)
    if formed % 2 == 0:
        prefix(1, TW)

    @pl.loop(0, (formed - 1) // 2)
    def _(i):
        t = 2 * i + 2 - formed % 2
        prefix(t, TW)
        prefix(t + 1, TW)

    for d in range(1, group):
        send(d).wait_send()
        recv(d).wait_recv()

    top = got[0, 0:2, :]
    for k in range(1, group):
        top = jnp.maximum(top, got[k, 0:2, :])
    total = jnp.zeros_like(top)
    lower = jnp.zeros_like(top)
    mass = jnp.zeros_like(top)
    for k in range(group):
        f = jnp.exp2(got[k, 0:2, :] - top)
        part = got[k, 2:4, :] * f
        total += part
        lower += part * jnp.where(k < me, 1.0, 0.0)
        mass += got[k, 4:6, :] * f
    inv = 1.0 / total
    pick_ref[...] = mass * inv
    low = lower * inv
    for half in range(rows // 128):
        r = pl.ds(half * 128, 128)
        fin_ref[0, r, :] = lanes_of(top[half:half + 1, :])
        fin_ref[1, r, :] = lanes_of(inv[half:half + 1, :])
        fin_ref[2, r, :] = lanes_of(low[half:half + 1, :])


def table(cfg, c_ref, mt_ref, fin_ref, mass_ref, out_hbm, pick_ref, stage, head_stage, tail_stage, off, tri, osem):
    rows, width = cfg
    n, widths, formed = tiling(width)
    slots = stage.shape[0]
    off[...] = fin_ref[2]
    pick_ref[...] = mass_ref[...]
    fill_triangle(tri)

    def slot_of(t):
        return lax.rem(t - 1, slots)

    def out_copy(t, w):
        buf = head_stage if w == FIRST else tail_stage if w == LAST else stage.at[slot_of(t)]
        sem = osem.at[slots] if w == FIRST else osem.at[slots + 1] if w == LAST else osem.at[slot_of(t)]
        col = 0 if w == FIRST else pl.multiple_of(start_of(t), 128)
        return pltpu.make_async_copy(buf, out_hbm.at[:, pl.ds(col, w)], sem)

    def finish(t, w, ready):
        buf = head_stage if w == FIRST else tail_stage if w == LAST else stage.at[slot_of(t)]
        for c, b in blocks_of(w):
            if not ready:
                buf[:, c:c + b] = block_prefix(c_ref[t, :, c:c + b], tri)
            for r0 in range(0, rows, RG):
                r = pl.ds(r0, RG)
                scale = jnp.exp2(mt_ref[t, r, :] - fin_ref[0, r, :]) * fin_ref[1, r, :]
                o = off[r, :]
                for g in range(c, c + b, 128):
                    v = c_ref[t, r, g:g + 128] if ready else buf[r, g:g + 128]
                    buf[r, g:g + 128] = v * scale + o
                off[r, :] = o + v[:, 127:128] * scale
        out_copy(t, w).start()

    def middle(lo, hi, ready):
        @pl.loop(lo, hi)
        def _(t):
            @pl.when(t > slots)
            def _():
                out_copy(t - slots, TW).wait()

            finish(t, TW, ready)

    finish(0, FIRST, True)
    middle(1, formed, True)
    middle(formed, n - 1, False)
    finish(n - 1, LAST, False)
    out_copy(0, FIRST).wait()
    for t in range(max(1, n - 1 - slots), n - 1):
        out_copy(t, TW).wait()
    out_copy(n - 1, LAST).wait()


def solution(mesh):
    vocab_axes = ("vblk", "vocab")
    nblk, nvoc = mesh.shape["vblk"], mesh.shape["vocab"]
    group = nblk * nvoc
    any_spec = pl.BlockSpec(memory_space=pl.ANY)
    vmem = pl.BlockSpec(memory_space=pltpu.VMEM)

    def local_step(hidden, w_head, inv_temp, target):
        rows, depth = hidden.shape
        width = w_head.shape[1]
        n = tiling(width)[0]
        halves = rows // 128
        e, mt, fin, mass = pl.pallas_call(
            functools.partial(head, (rows, width, nblk, nvoc)),
            name="head",
            out_shape=[
                pltpu.VMEM((n, rows, TW), F32),
                pltpu.VMEM((n, rows, 128), F32),
                pltpu.VMEM((3, rows, 128), F32),
                pltpu.VMEM((halves, 128), F32),
            ],
            in_specs=[any_spec, any_spec, vmem, vmem],
            out_specs=[vmem, vmem, vmem, vmem],
            scratch_shapes=[
                pltpu.VMEM((rows, depth), BF16),
                pltpu.VMEM((NBUF, depth, TW), BF16),
                pltpu.VMEM((rows, TW), F32),
                pltpu.VMEM((rows, TW), F32),
                pltpu.VMEM((rows, 128), F32),
                pltpu.VMEM((rows, 128), jnp.int32),
                pltpu.VMEM((rows, 128), F32),
                pltpu.VMEM((rows, 128), F32),
                pltpu.VMEM((rows, 128), F32),
                pltpu.VMEM((BW, BW), BF16),
                pltpu.VMEM((8, 128), F32),
                pltpu.VMEM((group, 8, 128), F32),
                pltpu.SemaphoreType.DMA,
                pltpu.SemaphoreType.DMA((NBUF,)),
                pltpu.SemaphoreType.DMA((group,)),
                pltpu.SemaphoreType.DMA((group,)),
            ],
            compiler_params=pltpu.CompilerParams(
                collective_id=0, has_side_effects=True,
                vmem_limit_bytes=36 * 1024 * 1024),
            cost_estimate=pl.CostEstimate(
                flops=2 * rows * depth * width, bytes_accessed=2 * depth * width, transcendentals=rows * width),
        )(hidden, w_head, inv_temp.reshape(halves, 128), target.reshape(halves, 128))
        cdf, pick = pl.pallas_call(
            functools.partial(table, (rows, width)),
            name="table",
            out_shape=[jax.ShapeDtypeStruct((rows, width), F32), jax.ShapeDtypeStruct((halves, 128), F32)],
            in_specs=[vmem] * 4,
            out_specs=[any_spec, vmem],
            scratch_shapes=[
                pltpu.VMEM((SLOTS, rows, TW), F32),
                pltpu.VMEM((rows, FIRST), F32),
                pltpu.VMEM((rows, LAST), F32),
                pltpu.VMEM((rows, 128), F32),
                pltpu.VMEM((BW, BW), BF16),
                pltpu.SemaphoreType.DMA((SLOTS + 2,)),
            ],
            compiler_params=pltpu.CompilerParams(vmem_limit_bytes=13 * 1024 * 1024),
            cost_estimate=pl.CostEstimate(
                flops=4 * rows * width, bytes_accessed=4 * rows * width, transcendentals=0),
        )(e, mt, fin, mass)
        return cdf, pick.reshape(rows)

    return jax.shard_map(local_step, mesh=mesh,
                         in_specs=(P("dp", None), P(None, vocab_axes), P("dp"), P("dp")),
                         out_specs=(P("dp", vocab_axes), P("dp")), check_vma=False)
```

```python
import functools

import jax
import jax.numpy as jnp
from jax import lax
from jax.experimental import pallas as pl
from jax.experimental.pallas import tpu as pltpu
from jax.sharding import PartitionSpec as P

F32 = jnp.float32
BF16 = jnp.bfloat16
TW = 1536
FIRST = 384
LAST = 256
BW = 256
SLOTS = 6
RB = 16
NBUF = 4
RG = 32
LOG2E = 1.4426950408889634
NEG = -1e30


def lanes_of(row):
    return jnp.transpose(jnp.broadcast_to(row, (128, 128)))


def row_of(col):
    return jnp.transpose(col)[0:1, :]


def split3(x):
    hi = x.astype(BF16)
    r = x - hi.astype(F32)
    mid = r.astype(BF16)
    lo = (r - mid.astype(F32)).astype(BF16)
    return hi, mid, lo


def block_prefix(x, tri):
    w = x.shape[1]
    t = tri[:w, :w]
    hi, mid, lo = split3(x)
    dot = functools.partial(jnp.dot, preferred_element_type=F32)
    return dot(lo, t) + dot(mid, t) + dot(hi, t)


def fill_triangle(tri):
    i = lax.broadcasted_iota(jnp.int32, (BW, BW), 0)
    j = lax.broadcasted_iota(jnp.int32, (BW, BW), 1)
    tri[...] = jnp.where(i <= j, 1.0, 0.0).astype(BF16)


def tiling(width):
    mid = (width - FIRST - LAST) // TW
    assert FIRST + LAST + mid * TW == width and mid % 2 == 0 and mid >= 2
    return mid + 2, [FIRST] + [TW] * mid + [LAST]


def start_of(t):
    return FIRST + (t - 1) * TW


def blocks_of(width):
    return [(c, min(BW, width - c)) for c in range(0, width, BW)]


def head(cfg, h_hbm, w_hbm, tau_ref, tgt_ref, e_ref, mt_ref, fin_ref, pick_ref,
         h_ref, wbuf, z0, z1, tau, rel, m, s, pk, tri, pay, got, hsem, wsem, send_sem, recv_sem):
    rows, width, nblk, nvoc = cfg
    n, widths = tiling(width)
    zs = (z0, z1)
    mi, mj = lax.axis_index("vblk"), lax.axis_index("vocab")
    me = mi * nvoc + mj
    group = nblk * nvoc

    def peer(d):
        p = lax.rem(me + d, group)
        return {"vblk": p // nvoc, "vocab": lax.rem(p, nvoc)}

    def w_copy(t, slot, w):
        col = 0 if w == FIRST else pl.multiple_of(start_of(t), 128)
        return pltpu.make_async_copy(w_hbm.at[:, pl.ds(col, w)], wbuf.at[slot, :, pl.ds(0, w)], wsem.at[slot])

    h_copy = pltpu.make_async_copy(h_hbm, h_ref, hsem)
    h_copy.start()
    for t in range(min(NBUF, n)):
        w_copy(t, t, widths[t]).start()

    barrier = pltpu.get_barrier_semaphore()
    for d in range(1, group):
        pl.semaphore_signal(barrier, inc=1, device_id=peer(d), device_id_type=pl.DeviceIdType.MESH)

    base = me * width
    for half in range(rows // 128):
        r = pl.ds(half * 128, 128)
        tau[r, :] = lanes_of(tau_ref[half:half + 1, :] * LOG2E)
        rel[r, :] = lanes_of(tgt_ref[half:half + 1, :] - base)
    m[...] = jnp.full_like(m, NEG)
    s[...] = jnp.zeros_like(s)
    pk[...] = jnp.zeros_like(pk)
    fill_triangle(tri)
    lane = lax.broadcasted_iota(jnp.int32, (RG, 128), 1)

    def process(z, t, w):
        for r0 in range(0, rows, RG):
            r = pl.ds(r0, RG)
            top = z[r, 0:128]
            for c in range(128, w, 128):
                top = jnp.maximum(top, z[r, c:c + 128])
            new = jnp.max(top, axis=1, keepdims=True) * tau[r, :]
            mt_ref[t, r, :] = jnp.maximum(m[r, :], new)
        for r0 in range(0, rows, RG):
            r = pl.ds(r0, RG)
            new, scale = mt_ref[t, r, :], tau[r, :]
            lim = rel[r, :] - (0 if w == FIRST else start_of(t))
            total, mass = None, None
            for c in range(0, w, 128):
                e = jnp.exp2(z[r, c:c + 128] * scale - new)
                e_ref[t, r, c:c + 128] = e
                part = jnp.where(lane + c <= lim, e, 0.0)
                total = e if total is None else total + e
                mass = part if mass is None else mass + part
            alpha = jnp.exp2(m[r, :] - new)
            s[r, :] = s[r, :] * alpha + total
            pk[r, :] = pk[r, :] * alpha + mass
            m[r, :] = new

    def logits(z, slot, w):
        dot = functools.partial(jnp.dot, preferred_element_type=F32)
        if w > BW:
            z[:, 0:w] = dot(h_ref[...], wbuf[slot, :, 0:w])
        else:
            k = h_ref.shape[1] // 2
            z[:, 0:w] = dot(h_ref[:, :k], wbuf[slot, :k, 0:w]) + dot(h_ref[:, k:], wbuf[slot, k:, 0:w])

    def step(t, parity):
        slot = lax.rem(t, NBUF)
        w_copy(t, slot, TW).wait()
        ahead = t + NBUF - 1

        @pl.when(ahead < n - 1)
        def _():
            w_copy(ahead, lax.rem(ahead, NBUF), TW).start()

        @pl.when(ahead == n - 1)
        def _():
            w_copy(n - 1, (n - 1) % NBUF, LAST).start()

        process(zs[1 - parity], t - 1, TW)
        logits(zs[parity], slot, TW)

    h_copy.wait()
    w_copy(0, 0, FIRST).wait()
    logits(z0, 0, FIRST)
    w_copy(1, 1, TW).wait()
    if NBUF < n:
        w_copy(NBUF, 0, widths[NBUF]).start()
    process(z0, 0, FIRST)
    logits(z1, 1, TW)

    @pl.loop(0, (n - 4) // 2)
    def _(i):
        step(2 * i + 2, 0)
        step(2 * i + 3, 1)

    w_copy(n - 2, (n - 2) % NBUF, TW).wait()
    process(z1, n - 3, TW)
    logits(z0, (n - 2) % NBUF, TW)
    w_copy(n - 1, (n - 1) % NBUF, LAST).wait()
    process(z0, n - 2, TW)
    logits(z1, (n - 1) % NBUF, LAST)
    process(z1, n - 1, LAST)

    for half in range(rows // 128):
        r = pl.ds(half * 128, 128)
        ones = jnp.zeros((128, 128), F32)
        pay[half:half + 1, :] = row_of(m[r, :])
        pay[2 + half:3 + half, :] = row_of(jnp.sum(s[r, :], axis=1, keepdims=True) + ones)
        pay[4 + half:5 + half, :] = row_of(jnp.sum(pk[r, :], axis=1, keepdims=True) + ones)
    pl.semaphore_wait(barrier, group - 1)

    def send(d):
        return pltpu.make_async_remote_copy(
            src_ref=pay.at[0:6], dst_ref=got.at[me, 0:6], send_sem=send_sem.at[d], recv_sem=recv_sem.at[me],
            device_id=peer(d), device_id_type=pl.DeviceIdType.MESH)

    def recv(d):
        k = lax.rem(me + d, group)
        return pltpu.make_async_remote_copy(
            src_ref=pay.at[0:6], dst_ref=got.at[k, 0:6], send_sem=send_sem.at[d], recv_sem=recv_sem.at[k],
            device_id=peer(d), device_id_type=pl.DeviceIdType.MESH)

    for d in sorted(range(1, group), key=lambda d: -min(d, group - d)):
        send(d).start()
    got[me, 0:6, :] = pay[0:6, :]

    def prefix(t, w):
        for c, b in blocks_of(w):
            e_ref[t, :, c:c + b] = block_prefix(e_ref[t, :, c:c + b], tri)

    prefix(0, FIRST)
    prefix(n - 1, LAST)

    @pl.loop(1, n - 1)
    def _(t):
        prefix(t, TW)

    for d in range(1, group):
        send(d).wait_send()
        recv(d).wait_recv()

    top = got[0, 0:2, :]
    for k in range(1, group):
        top = jnp.maximum(top, got[k, 0:2, :])
    total = jnp.zeros_like(top)
    lower = jnp.zeros_like(top)
    mass = jnp.zeros_like(top)
    for k in range(group):
        f = jnp.exp2(got[k, 0:2, :] - top)
        part = got[k, 2:4, :] * f
        total += part
        lower += part * jnp.where(k < me, 1.0, 0.0)
        mass += got[k, 4:6, :] * f
    inv = 1.0 / total
    pick_ref[...] = mass * inv
    low = lower * inv
    for half in range(rows // 128):
        r = pl.ds(half * 128, 128)
        fin_ref[0, r, :] = lanes_of(top[half:half + 1, :])
        fin_ref[1, r, :] = lanes_of(inv[half:half + 1, :])
        fin_ref[2, r, :] = lanes_of(low[half:half + 1, :])


def table(cfg, c_ref, mt_ref, fin_ref, mass_ref, out_hbm, pick_ref, stage, osem):
    rows, width = cfg
    n, widths = tiling(width)
    steps = rows // RB
    pick_ref[...] = mass_ref[...]

    def out_copy(i):
        slot = lax.rem(i, SLOTS)
        return pltpu.make_async_copy(
            stage.at[slot], out_hbm.at[pl.ds(pl.multiple_of(i * RB, RB), RB), :], osem.at[slot])

    @pl.loop(0, steps)
    def _(i):
        slot = lax.rem(i, SLOTS)

        @pl.when(i >= SLOTS)
        def _():
            out_copy(i - SLOTS).wait()

        r = pl.ds(pl.multiple_of(i * RB, RB), RB)
        top, inv, off = fin_ref[0, r, :], fin_ref[1, r, :], fin_ref[2, r, :]
        col = 0
        for t in range(n):
            scale = jnp.exp2(mt_ref[t, r, :] - top) * inv
            for c, b in blocks_of(widths[t]):
                for g in range(c, c + b, 128):
                    v = c_ref[t, r, g:g + 128] * scale
                    stage[slot, :, col:col + 128] = v + off
                    col += 128
                off = off + v[:, 127:128]
        out_copy(i).start()

    for i in range(max(0, steps - SLOTS), steps):
        out_copy(i).wait()


def solution(mesh):
    vocab_axes = ("vblk", "vocab")
    nblk, nvoc = mesh.shape["vblk"], mesh.shape["vocab"]
    group = nblk * nvoc
    any_spec = pl.BlockSpec(memory_space=pl.ANY)
    vmem = pl.BlockSpec(memory_space=pltpu.VMEM)

    def local_step(hidden, w_head, inv_temp, target):
        rows, depth = hidden.shape
        width = w_head.shape[1]
        n = tiling(width)[0]
        halves = rows // 128
        e, mt, fin, mass = pl.pallas_call(
            functools.partial(head, (rows, width, nblk, nvoc)),
            name="head",
            out_shape=[
                pltpu.VMEM((n, rows, TW), F32),
                pltpu.VMEM((n, rows, 128), F32),
                pltpu.VMEM((3, rows, 128), F32),
                pltpu.VMEM((halves, 128), F32),
            ],
            in_specs=[any_spec, any_spec, vmem, vmem],
            out_specs=[vmem, vmem, vmem, vmem],
            scratch_shapes=[
                pltpu.VMEM((rows, depth), BF16),
                pltpu.VMEM((NBUF, depth, TW), BF16),
                pltpu.VMEM((rows, TW), F32),
                pltpu.VMEM((rows, TW), F32),
                pltpu.VMEM((rows, 128), F32),
                pltpu.VMEM((rows, 128), jnp.int32),
                pltpu.VMEM((rows, 128), F32),
                pltpu.VMEM((rows, 128), F32),
                pltpu.VMEM((rows, 128), F32),
                pltpu.VMEM((BW, BW), BF16),
                pltpu.VMEM((8, 128), F32),
                pltpu.VMEM((group, 8, 128), F32),
                pltpu.SemaphoreType.DMA,
                pltpu.SemaphoreType.DMA((NBUF,)),
                pltpu.SemaphoreType.DMA((group,)),
                pltpu.SemaphoreType.DMA((group,)),
            ],
            compiler_params=pltpu.CompilerParams(
                collective_id=0, has_side_effects=True,
                vmem_limit_bytes=38 * 1024 * 1024),
            cost_estimate=pl.CostEstimate(
                flops=2 * rows * depth * width, bytes_accessed=2 * depth * width, transcendentals=rows * width),
        )(hidden, w_head, inv_temp.reshape(halves, 128), target.reshape(halves, 128))
        cdf, pick = pl.pallas_call(
            functools.partial(table, (rows, width)),
            name="table",
            out_shape=[jax.ShapeDtypeStruct((rows, width), F32), jax.ShapeDtypeStruct((halves, 128), F32)],
            in_specs=[vmem] * 4,
            out_specs=[any_spec, vmem],
            scratch_shapes=[
                pltpu.VMEM((SLOTS, RB, width), F32),
                pltpu.SemaphoreType.DMA((SLOTS,)),
            ],
            compiler_params=pltpu.CompilerParams(vmem_limit_bytes=9 * 1024 * 1024),
            cost_estimate=pl.CostEstimate(
                flops=4 * rows * width, bytes_accessed=4 * rows * width, transcendentals=0),
        )(e, mt, fin, mass)
        return cdf, pick.reshape(rows)

    return jax.shard_map(local_step, mesh=mesh,
                         in_specs=(P("dp", None), P(None, vocab_axes), P("dp"), P("dp")),
                         out_specs=(P("dp", vocab_axes), P("dp")), check_vma=False)
```

```python
import functools

import jax
import jax.numpy as jnp
from jax import lax
from jax.experimental import pallas as pl
from jax.experimental.pallas import tpu as pltpu
from jax.sharding import PartitionSpec as P

F32 = jnp.float32
BF16 = jnp.bfloat16
TW = 1024
FIRST = 384
LAST = 256
BW = 256
HEAD_MID = 12
SLOTS = 6
RB = 16
NBUF = 4
RG = 32
LOG2E = 1.4426950408889634
NEG = -1e30


def lanes_of(row):
    return jnp.transpose(jnp.broadcast_to(row, (128, 128)))


def row_of(col):
    return jnp.transpose(col)[0:1, :]


def split3(x):
    hi = x.astype(BF16)
    r = x - hi.astype(F32)
    mid = r.astype(BF16)
    lo = (r - mid.astype(F32)).astype(BF16)
    return hi, mid, lo


def block_prefix(x, tri):
    w = x.shape[1]
    t = tri[:w, :w]
    hi, mid, lo = split3(x)
    dot = functools.partial(jnp.dot, preferred_element_type=F32)
    return dot(lo, t) + dot(mid, t) + dot(hi, t)


def fill_triangle(tri):
    i = lax.broadcasted_iota(jnp.int32, (BW, BW), 0)
    j = lax.broadcasted_iota(jnp.int32, (BW, BW), 1)
    tri[...] = jnp.where(i <= j, 1.0, 0.0).astype(BF16)


def tiling(width):
    mid = (width - FIRST - LAST) // TW
    assert FIRST + LAST + mid * TW == width and mid % 2 == 1
    return mid + 2, [FIRST] + [TW] * mid + [LAST], 1 + mid * HEAD_MID // 15


def start_of(t):
    return FIRST + (t - 1) * TW


def blocks_of(width):
    return [(c, min(BW, width - c)) for c in range(0, width, BW)]


def head(cfg, h_hbm, w_hbm, tau_ref, tgt_ref, e_ref, mt_ref, fin_ref, pick_ref,
         h_ref, wbuf, z0, z1, tau, rel, m, s, pk, tri, pay, got, hsem, wsem, send_sem, recv_sem):
    rows, width, nblk, nvoc = cfg
    n, widths, formed = tiling(width)
    zs = (z0, z1)
    mi, mj = lax.axis_index("vblk"), lax.axis_index("vocab")
    me = mi * nvoc + mj
    group = nblk * nvoc

    def peer(d):
        p = lax.rem(me + d, group)
        return {"vblk": p // nvoc, "vocab": lax.rem(p, nvoc)}

    def w_copy(t, slot, w):
        col = 0 if w == FIRST else pl.multiple_of(start_of(t), 128)
        return pltpu.make_async_copy(w_hbm.at[:, pl.ds(col, w)], wbuf.at[slot, :, pl.ds(0, w)], wsem.at[slot])

    h_copy = pltpu.make_async_copy(h_hbm, h_ref, hsem)
    h_copy.start()
    for t in range(min(NBUF, n)):
        w_copy(t, t, widths[t]).start()

    barrier = pltpu.get_barrier_semaphore()
    for d in range(1, group):
        pl.semaphore_signal(barrier, inc=1, device_id=peer(d), device_id_type=pl.DeviceIdType.MESH)

    base = me * width
    for half in range(rows // 128):
        r = pl.ds(half * 128, 128)
        tau[r, :] = lanes_of(tau_ref[half:half + 1, :] * LOG2E)
        rel[r, :] = lanes_of(tgt_ref[half:half + 1, :] - base)
    m[...] = jnp.full_like(m, NEG)
    s[...] = jnp.zeros_like(s)
    pk[...] = jnp.zeros_like(pk)
    fill_triangle(tri)
    lane = lax.broadcasted_iota(jnp.int32, (RG, 128), 1)

    def process(z, t, w):
        for r0 in range(0, rows, RG):
            r = pl.ds(r0, RG)
            top = z[r, 0:128]
            for c in range(128, w, 128):
                top = jnp.maximum(top, z[r, c:c + 128])
            new = jnp.max(top, axis=1, keepdims=True) * tau[r, :]
            mt_ref[t, r, :] = jnp.maximum(m[r, :], new)
        for r0 in range(0, rows, RG):
            r = pl.ds(r0, RG)
            new, scale = mt_ref[t, r, :], tau[r, :]
            lim = rel[r, :] - (0 if w == FIRST else start_of(t))
            total, mass = None, None
            for c in range(0, w, 128):
                e = jnp.exp2(z[r, c:c + 128] * scale - new)
                e_ref[t, r, c:c + 128] = e
                part = jnp.where(lane + c <= lim, e, 0.0)
                total = e if total is None else total + e
                mass = part if mass is None else mass + part
            alpha = jnp.exp2(m[r, :] - new)
            s[r, :] = s[r, :] * alpha + total
            pk[r, :] = pk[r, :] * alpha + mass
            m[r, :] = new

    def logits(z, slot, w):
        dot = functools.partial(jnp.dot, preferred_element_type=F32)
        if w > BW:
            z[:, 0:w] = dot(h_ref[...], wbuf[slot, :, 0:w])
        else:
            k = h_ref.shape[1] // 2
            z[:, 0:w] = dot(h_ref[:, :k], wbuf[slot, :k, 0:w]) + dot(h_ref[:, k:], wbuf[slot, k:, 0:w])

    def step(t, parity):
        slot = lax.rem(t, NBUF)
        w_copy(t, slot, TW).wait()
        ahead = t + NBUF - 1

        @pl.when(ahead < n - 1)
        def _():
            w_copy(ahead, lax.rem(ahead, NBUF), TW).start()

        @pl.when(ahead == n - 1)
        def _():
            w_copy(n - 1, (n - 1) % NBUF, LAST).start()

        process(zs[1 - parity], t - 1, TW)
        logits(zs[parity], slot, TW)

    h_copy.wait()
    w_copy(0, 0, FIRST).wait()
    logits(z0, 0, FIRST)
    w_copy(1, 1, TW).wait()
    if NBUF < n:
        w_copy(NBUF, 0, widths[NBUF]).start()
    process(z0, 0, FIRST)
    logits(z1, 1, TW)

    @pl.loop(0, (n - 3) // 2)
    def _(i):
        step(2 * i + 2, 0)
        step(2 * i + 3, 1)

    w_copy(n - 1, (n - 1) % NBUF, LAST).wait()
    process(zs[n % 2], n - 2, TW)
    logits(zs[(n - 1) % 2], (n - 1) % NBUF, LAST)
    process(zs[(n - 1) % 2], n - 1, LAST)

    for half in range(rows // 128):
        r = pl.ds(half * 128, 128)
        ones = jnp.zeros((128, 128), F32)
        pay[half:half + 1, :] = row_of(m[r, :])
        pay[2 + half:3 + half, :] = row_of(jnp.sum(s[r, :], axis=1, keepdims=True) + ones)
        pay[4 + half:5 + half, :] = row_of(jnp.sum(pk[r, :], axis=1, keepdims=True) + ones)
    pl.semaphore_wait(barrier, group - 1)

    def send(d):
        return pltpu.make_async_remote_copy(
            src_ref=pay.at[0:6], dst_ref=got.at[me, 0:6], send_sem=send_sem.at[d], recv_sem=recv_sem.at[me],
            device_id=peer(d), device_id_type=pl.DeviceIdType.MESH)

    def recv(d):
        k = lax.rem(me + d, group)
        return pltpu.make_async_remote_copy(
            src_ref=pay.at[0:6], dst_ref=got.at[k, 0:6], send_sem=send_sem.at[d], recv_sem=recv_sem.at[k],
            device_id=peer(d), device_id_type=pl.DeviceIdType.MESH)

    for d in range(1, group):
        send(d).start()
    got[me, 0:6, :] = pay[0:6, :]

    def prefix(t, w):
        for c, b in blocks_of(w):
            e_ref[t, :, c:c + b] = block_prefix(e_ref[t, :, c:c + b], tri)

    prefix(0, FIRST)
    if formed % 2 == 0:
        prefix(1, TW)

    @pl.loop(0, (formed - 1) // 2)
    def _(i):
        t = 2 * i + 2 - formed % 2
        prefix(t, TW)
        prefix(t + 1, TW)

    for d in range(1, group):
        send(d).wait_send()
        recv(d).wait_recv()

    top = got[0, 0:2, :]
    for k in range(1, group):
        top = jnp.maximum(top, got[k, 0:2, :])
    total = jnp.zeros_like(top)
    lower = jnp.zeros_like(top)
    mass = jnp.zeros_like(top)
    for k in range(group):
        f = jnp.exp2(got[k, 0:2, :] - top)
        part = got[k, 2:4, :] * f
        total += part
        lower += part * jnp.where(k < me, 1.0, 0.0)
        mass += got[k, 4:6, :] * f
    inv = 1.0 / total
    pick_ref[...] = mass * inv
    low = lower * inv
    for half in range(rows // 128):
        r = pl.ds(half * 128, 128)
        fin_ref[0, r, :] = lanes_of(top[half:half + 1, :])
        fin_ref[1, r, :] = lanes_of(inv[half:half + 1, :])
        fin_ref[2, r, :] = lanes_of(low[half:half + 1, :])


def table(cfg, c_ref, mt_ref, fin_ref, mass_ref, out_hbm, pick_ref, stage, tri, osem):
    rows, width = cfg
    n, widths, formed = tiling(width)
    steps = rows // RB
    pick_ref[...] = mass_ref[...]
    fill_triangle(tri)
    late = [(t, c) for t in range(formed, n) for c, _ in blocks_of(widths[t])]

    def out_copy(i):
        slot = lax.rem(i, SLOTS)
        return pltpu.make_async_copy(
            stage.at[slot], out_hbm.at[pl.ds(pl.multiple_of(i * RB, RB), RB), :], osem.at[slot])

    @pl.loop(0, steps)
    def _(i):
        slot = lax.rem(i, SLOTS)

        @pl.when(i >= SLOTS)
        def _():
            out_copy(i - SLOTS).wait()

        r = pl.ds(pl.multiple_of(i * RB, RB), RB)
        top, inv, off = fin_ref[0, r, :], fin_ref[1, r, :], fin_ref[2, r, :]
        x = jnp.concatenate([c_ref[t, r, c:c + BW] for t, c in late], axis=0)
        hi, mid, lo = split3(x)
        y = jnp.dot(jnp.concatenate([lo, mid, hi], axis=0), tri[...], preferred_element_type=F32)
        k = x.shape[0]
        y = y[:k] + y[k:2 * k] + y[2 * k:]
        col = 0
        for t in range(n):
            scale = jnp.exp2(mt_ref[t, r, :] - top) * inv
            for c, b in blocks_of(widths[t]):
                for g in range(c, c + b, 128):
                    if t < formed:
                        v = c_ref[t, r, g:g + 128] * scale
                    else:
                        j = late.index((t, c)) * RB
                        v = y[j:j + RB, g - c:g - c + 128] * scale
                    stage[slot, :, col:col + 128] = v + off
                    col += 128
                off = off + v[:, 127:128]
        out_copy(i).start()

    for i in range(max(0, steps - SLOTS), steps):
        out_copy(i).wait()


def solution(mesh):
    vocab_axes = ("vblk", "vocab")
    nblk, nvoc = mesh.shape["vblk"], mesh.shape["vocab"]
    group = nblk * nvoc
    any_spec = pl.BlockSpec(memory_space=pl.ANY)
    vmem = pl.BlockSpec(memory_space=pltpu.VMEM)

    def local_step(hidden, w_head, inv_temp, target):
        rows, depth = hidden.shape
        width = w_head.shape[1]
        n = tiling(width)[0]
        halves = rows // 128
        e, mt, fin, mass = pl.pallas_call(
            functools.partial(head, (rows, width, nblk, nvoc)),
            name="head",
            out_shape=[
                pltpu.VMEM((n, rows, TW), F32),
                pltpu.VMEM((n, rows, 128), F32),
                pltpu.VMEM((3, rows, 128), F32),
                pltpu.VMEM((halves, 128), F32),
            ],
            in_specs=[any_spec, any_spec, vmem, vmem],
            out_specs=[vmem, vmem, vmem, vmem],
            scratch_shapes=[
                pltpu.VMEM((rows, depth), BF16),
                pltpu.VMEM((NBUF, depth, TW), BF16),
                pltpu.VMEM((rows, TW), F32),
                pltpu.VMEM((rows, TW), F32),
                pltpu.VMEM((rows, 128), F32),
                pltpu.VMEM((rows, 128), jnp.int32),
                pltpu.VMEM((rows, 128), F32),
                pltpu.VMEM((rows, 128), F32),
                pltpu.VMEM((rows, 128), F32),
                pltpu.VMEM((BW, BW), BF16),
                pltpu.VMEM((8, 128), F32),
                pltpu.VMEM((group, 8, 128), F32),
                pltpu.SemaphoreType.DMA,
                pltpu.SemaphoreType.DMA((NBUF,)),
                pltpu.SemaphoreType.DMA((group,)),
                pltpu.SemaphoreType.DMA((group,)),
            ],
            compiler_params=pltpu.CompilerParams(
                collective_id=0, has_side_effects=True,
                vmem_limit_bytes=36 * 1024 * 1024),
            cost_estimate=pl.CostEstimate(
                flops=2 * rows * depth * width, bytes_accessed=2 * depth * width, transcendentals=rows * width),
        )(hidden, w_head, inv_temp.reshape(halves, 128), target.reshape(halves, 128))
        cdf, pick = pl.pallas_call(
            functools.partial(table, (rows, width)),
            name="table",
            out_shape=[jax.ShapeDtypeStruct((rows, width), F32), jax.ShapeDtypeStruct((halves, 128), F32)],
            in_specs=[vmem] * 4,
            out_specs=[any_spec, vmem],
            scratch_shapes=[
                pltpu.VMEM((SLOTS, RB, width), F32),
                pltpu.VMEM((BW, BW), BF16),
                pltpu.SemaphoreType.DMA((SLOTS,)),
            ],
            compiler_params=pltpu.CompilerParams(vmem_limit_bytes=10 * 1024 * 1024),
            cost_estimate=pl.CostEstimate(
                flops=4 * rows * width, bytes_accessed=4 * rows * width, transcendentals=0),
        )(e, mt, fin, mass)
        return cdf, pick.reshape(rows)

    return jax.shard_map(local_step, mesh=mesh,
                         in_specs=(P("dp", None), P(None, vocab_axes), P("dp"), P("dp")),
                         out_specs=(P("dp", vocab_axes), P("dp")), check_vma=False)
```

```python
import functools

import jax
import jax.numpy as jnp
from jax import lax
from jax.experimental import pallas as pl
from jax.experimental.pallas import tpu as pltpu
from jax.sharding import PartitionSpec as P

F32 = jnp.float32
BF16 = jnp.bfloat16
TW = 1024
FIRST = 384
LAST = 256
BW = 256
HEAD_MID = 14
SLOTS = 6
RB = 16
NBUF = 4
AHEAD = 2
RG = 32
LOG2E = 1.4426950408889634
NEG = -1e30


def lanes_of(row):
    return jnp.transpose(jnp.broadcast_to(row, (128, 128)))


def row_of(col):
    return jnp.transpose(col)[0:1, :]


def split3(x):
    hi = x.astype(BF16)
    r = x - hi.astype(F32)
    mid = r.astype(BF16)
    lo = (r - mid.astype(F32)).astype(BF16)
    return hi, mid, lo


def block_prefix(x, tri):
    w = x.shape[1]
    t = tri[:w, :w]
    hi, mid, lo = split3(x)
    dot = functools.partial(jnp.dot, preferred_element_type=F32)
    return dot(lo, t) + dot(mid, t) + dot(hi, t)


def fill_triangle(tri):
    i = lax.broadcasted_iota(jnp.int32, (BW, BW), 0)
    j = lax.broadcasted_iota(jnp.int32, (BW, BW), 1)
    tri[...] = jnp.where(i <= j, 1.0, 0.0).astype(BF16)


def tiling(width):
    mid = (width - FIRST - LAST) // TW
    assert FIRST + LAST + mid * TW == width and mid % 2 == 1
    return mid + 2, [FIRST] + [TW] * mid + [LAST], 1 + mid * HEAD_MID // 15


def start_of(t):
    return FIRST + (t - 1) * TW


def blocks_of(width):
    return [(c, min(BW, width - c)) for c in range(0, width, BW)]


def head(cfg, h_hbm, w_hbm, tau_ref, tgt_ref, e_ref, mt_ref, fin_ref, pick_ref,
         h_ref, wbuf, z0, z1, tau, rel, m, s, pk, tri, pay, got, hsem, wsem, send_sem, recv_sem):
    rows, width, nblk, nvoc = cfg
    n, widths, formed = tiling(width)
    zs = (z0, z1)
    mi, mj = lax.axis_index("vblk"), lax.axis_index("vocab")
    me = mi * nvoc + mj
    group = nblk * nvoc

    def peer(d):
        p = lax.rem(me + d, group)
        return {"vblk": p // nvoc, "vocab": lax.rem(p, nvoc)}

    def w_copy(t, slot, w):
        col = 0 if w == FIRST else pl.multiple_of(start_of(t), 128)
        return pltpu.make_async_copy(w_hbm.at[:, pl.ds(col, w)], wbuf.at[slot, :, pl.ds(0, w)], wsem.at[slot])

    h_copy = pltpu.make_async_copy(h_hbm, h_ref, hsem)
    h_copy.start()
    for t in range(AHEAD):
        w_copy(t, t, widths[t]).start()

    barrier = pltpu.get_barrier_semaphore()
    for d in range(1, group):
        pl.semaphore_signal(barrier, inc=1, device_id=peer(d), device_id_type=pl.DeviceIdType.MESH)

    base = me * width
    for half in range(rows // 128):
        r = pl.ds(half * 128, 128)
        tau[r, :] = lanes_of(tau_ref[half:half + 1, :] * LOG2E)
        rel[r, :] = lanes_of(tgt_ref[half:half + 1, :] - base)
    m[...] = jnp.full_like(m, NEG)
    s[...] = jnp.zeros_like(s)
    pk[...] = jnp.zeros_like(pk)
    fill_triangle(tri)
    lane = lax.broadcasted_iota(jnp.int32, (RG, 128), 1)

    def process(z, t, w):
        for r0 in range(0, rows, RG):
            r = pl.ds(r0, RG)
            top = z[r, 0:128]
            for c in range(128, w, 128):
                top = jnp.maximum(top, z[r, c:c + 128])
            new = jnp.max(top, axis=1, keepdims=True) * tau[r, :]
            mt_ref[t, r, :] = jnp.maximum(m[r, :], new)
        for r0 in range(0, rows, RG):
            r = pl.ds(r0, RG)
            new, scale = mt_ref[t, r, :], tau[r, :]
            lim = rel[r, :] - (0 if w == FIRST else start_of(t))
            total, mass = None, None
            for c in range(0, w, 128):
                e = jnp.exp2(z[r, c:c + 128] * scale - new)
                e_ref[t, r, c:c + 128] = e
                part = jnp.where(lane + c <= lim, e, 0.0)
                total = e if total is None else total + e
                mass = part if mass is None else mass + part
            alpha = jnp.exp2(m[r, :] - new)
            s[r, :] = s[r, :] * alpha + total
            pk[r, :] = pk[r, :] * alpha + mass
            m[r, :] = new

    def logits(z, slot, w):
        dot = functools.partial(jnp.dot, preferred_element_type=F32)
        if w > BW:
            z[:, 0:w] = dot(h_ref[...], wbuf[slot, :, 0:w])
        else:
            k = h_ref.shape[1] // 2
            z[:, 0:w] = dot(h_ref[:, :k], wbuf[slot, :k, 0:w]) + dot(h_ref[:, k:], wbuf[slot, k:, 0:w])

    def step(t, parity):
        slot = lax.rem(t, NBUF)
        w_copy(t, slot, TW).wait()
        ahead = t + AHEAD

        @pl.when(ahead < n - 1)
        def _():
            w_copy(ahead, lax.rem(ahead, NBUF), TW).start()

        @pl.when(ahead == n - 1)
        def _():
            w_copy(n - 1, (n - 1) % NBUF, LAST).start()

        process(zs[1 - parity], t - 1, TW)
        logits(zs[parity], slot, TW)

    h_copy.wait()
    w_copy(0, 0, FIRST).wait()
    w_copy(AHEAD, AHEAD, TW).start()
    logits(z0, 0, FIRST)
    w_copy(1, 1, TW).wait()
    w_copy(AHEAD + 1, AHEAD + 1, TW).start()
    process(z0, 0, FIRST)
    logits(z1, 1, TW)

    @pl.loop(0, (n - 3) // 2)
    def _(i):
        step(2 * i + 2, 0)
        step(2 * i + 3, 1)

    w_copy(n - 1, (n - 1) % NBUF, LAST).wait()
    process(zs[n % 2], n - 2, TW)
    logits(zs[(n - 1) % 2], (n - 1) % NBUF, LAST)
    process(zs[(n - 1) % 2], n - 1, LAST)

    for half in range(rows // 128):
        r = pl.ds(half * 128, 128)
        ones = jnp.zeros((128, 128), F32)
        pay[half:half + 1, :] = row_of(m[r, :])
        pay[2 + half:3 + half, :] = row_of(jnp.sum(s[r, :], axis=1, keepdims=True) + ones)
        pay[4 + half:5 + half, :] = row_of(jnp.sum(pk[r, :], axis=1, keepdims=True) + ones)
    pl.semaphore_wait(barrier, group - 1)

    def send(d):
        return pltpu.make_async_remote_copy(
            src_ref=pay.at[0:6], dst_ref=got.at[me, 0:6], send_sem=send_sem.at[d], recv_sem=recv_sem.at[me],
            device_id=peer(d), device_id_type=pl.DeviceIdType.MESH)

    def recv(d):
        k = lax.rem(me + d, group)
        return pltpu.make_async_remote_copy(
            src_ref=pay.at[0:6], dst_ref=got.at[k, 0:6], send_sem=send_sem.at[d], recv_sem=recv_sem.at[k],
            device_id=peer(d), device_id_type=pl.DeviceIdType.MESH)

    for d in range(1, group):
        send(d).start()
    got[me, 0:6, :] = pay[0:6, :]

    def prefix(t, w):
        for c, b in blocks_of(w):
            e_ref[t, :, c:c + b] = block_prefix(e_ref[t, :, c:c + b], tri)

    prefix(0, FIRST)
    if formed % 2 == 0:
        prefix(1, TW)

    @pl.loop(0, (formed - 1) // 2)
    def _(i):
        t = 2 * i + 2 - formed % 2
        prefix(t, TW)
        prefix(t + 1, TW)

    for d in range(1, group):
        send(d).wait_send()
        recv(d).wait_recv()

    top = got[0, 0:2, :]
    for k in range(1, group):
        top = jnp.maximum(top, got[k, 0:2, :])
    total = jnp.zeros_like(top)
    lower = jnp.zeros_like(top)
    mass = jnp.zeros_like(top)
    for k in range(group):
        f = jnp.exp2(got[k, 0:2, :] - top)
        part = got[k, 2:4, :] * f
        total += part
        lower += part * jnp.where(k < me, 1.0, 0.0)
        mass += got[k, 4:6, :] * f
    inv = 1.0 / total
    pick_ref[...] = mass * inv
    low = lower * inv
    for half in range(rows // 128):
        r = pl.ds(half * 128, 128)
        fin_ref[0, r, :] = lanes_of(top[half:half + 1, :])
        fin_ref[1, r, :] = lanes_of(inv[half:half + 1, :])
        fin_ref[2, r, :] = lanes_of(low[half:half + 1, :])


def table(cfg, c_ref, mt_ref, fin_ref, mass_ref, out_hbm, pick_ref, stage, tri, osem):
    rows, width = cfg
    n, widths, formed = tiling(width)
    steps = rows // RB
    pick_ref[...] = mass_ref[...]
    fill_triangle(tri)
    late = [(t, c) for t in range(formed, n) for c, _ in blocks_of(widths[t])]

    def out_copy(i):
        slot = lax.rem(i, SLOTS)
        return pltpu.make_async_copy(
            stage.at[slot], out_hbm.at[pl.ds(pl.multiple_of(i * RB, RB), RB), :], osem.at[slot])

    @pl.loop(0, steps)
    def _(i):
        slot = lax.rem(i, SLOTS)

        @pl.when(i >= SLOTS)
        def _():
            out_copy(i - SLOTS).wait()

        r = pl.ds(pl.multiple_of(i * RB, RB), RB)
        top, inv, off = fin_ref[0, r, :], fin_ref[1, r, :], fin_ref[2, r, :]
        x = jnp.concatenate([c_ref[t, r, c:c + BW] for t, c in late], axis=0)
        hi, mid, lo = split3(x)
        y = jnp.dot(jnp.concatenate([lo, mid, hi], axis=0), tri[...], preferred_element_type=F32)
        k = x.shape[0]
        y = y[:k] + y[k:2 * k] + y[2 * k:]
        col = 0
        for t in range(n):
            scale = jnp.exp2(mt_ref[t, r, :] - top) * inv
            for c, b in blocks_of(widths[t]):
                for g in range(c, c + b, 128):
                    if t < formed:
                        v = c_ref[t, r, g:g + 128] * scale
                    else:
                        j = late.index((t, c)) * RB
                        v = y[j:j + RB, g - c:g - c + 128] * scale
                    stage[slot, :, col:col + 128] = v + off
                    col += 128
                off = off + v[:, 127:128]
        out_copy(i).start()

    for i in range(max(0, steps - SLOTS), steps):
        out_copy(i).wait()


def solution(mesh):
    vocab_axes = ("vblk", "vocab")
    nblk, nvoc = mesh.shape["vblk"], mesh.shape["vocab"]
    group = nblk * nvoc
    any_spec = pl.BlockSpec(memory_space=pl.ANY)
    vmem = pl.BlockSpec(memory_space=pltpu.VMEM)

    def local_step(hidden, w_head, inv_temp, target):
        rows, depth = hidden.shape
        width = w_head.shape[1]
        n = tiling(width)[0]
        halves = rows // 128
        e, mt, fin, mass = pl.pallas_call(
            functools.partial(head, (rows, width, nblk, nvoc)),
            name="head",
            out_shape=[
                pltpu.VMEM((n, rows, TW), F32),
                pltpu.VMEM((n, rows, 128), F32),
                pltpu.VMEM((3, rows, 128), F32),
                pltpu.VMEM((halves, 128), F32),
            ],
            in_specs=[any_spec, any_spec, vmem, vmem],
            out_specs=[vmem, vmem, vmem, vmem],
            scratch_shapes=[
                pltpu.VMEM((rows, depth), BF16),
                pltpu.VMEM((NBUF, depth, TW), BF16),
                pltpu.VMEM((rows, TW), F32),
                pltpu.VMEM((rows, TW), F32),
                pltpu.VMEM((rows, 128), F32),
                pltpu.VMEM((rows, 128), jnp.int32),
                pltpu.VMEM((rows, 128), F32),
                pltpu.VMEM((rows, 128), F32),
                pltpu.VMEM((rows, 128), F32),
                pltpu.VMEM((BW, BW), BF16),
                pltpu.VMEM((8, 128), F32),
                pltpu.VMEM((group, 8, 128), F32),
                pltpu.SemaphoreType.DMA,
                pltpu.SemaphoreType.DMA((NBUF,)),
                pltpu.SemaphoreType.DMA((group,)),
                pltpu.SemaphoreType.DMA((group,)),
            ],
            compiler_params=pltpu.CompilerParams(
                collective_id=0, has_side_effects=True,
                vmem_limit_bytes=36 * 1024 * 1024),
            cost_estimate=pl.CostEstimate(
                flops=2 * rows * depth * width, bytes_accessed=2 * depth * width, transcendentals=rows * width),
        )(hidden, w_head, inv_temp.reshape(halves, 128), target.reshape(halves, 128))
        cdf, pick = pl.pallas_call(
            functools.partial(table, (rows, width)),
            name="table",
            out_shape=[jax.ShapeDtypeStruct((rows, width), F32), jax.ShapeDtypeStruct((halves, 128), F32)],
            in_specs=[vmem] * 4,
            out_specs=[any_spec, vmem],
            scratch_shapes=[
                pltpu.VMEM((SLOTS, RB, width), F32),
                pltpu.VMEM((BW, BW), BF16),
                pltpu.SemaphoreType.DMA((SLOTS,)),
            ],
            compiler_params=pltpu.CompilerParams(vmem_limit_bytes=10 * 1024 * 1024),
            cost_estimate=pl.CostEstimate(
                flops=4 * rows * width, bytes_accessed=4 * rows * width, transcendentals=0),
        )(e, mt, fin, mass)
        return cdf, pick.reshape(rows)

    return jax.shard_map(local_step, mesh=mesh,
                         in_specs=(P("dp", None), P(None, vocab_axes), P("dp"), P("dp")),
                         out_specs=(P("dp", vocab_axes), P("dp")), check_vma=False)
```
